512 devices in a mesh: pat: 2 (over y), slab: 32 (over z), phase: 4 (over x), enc: 2 (over core).
Axes of the slice: x: 4, y: 2, z: 32, core: 2. Of those that a mesh axis runs over, the one named last changes fastest.
The devices are a block of a 4x8x32 slice.
Arguments:
- kspace_data: bfloat16 [4, 4, 4, 96, 64, 192], P('pat', 'phase', 'enc', 'slab'), parts along dimension 0, may hold values from -6 to 6
- coil_maps: bfloat16 [4, 24, 4, 64, 192], P('pat', None, None, 'slab'), parts along dimension 0, may hold values from -1 to 1
- sampling: int32 [4, 4, 128, 192], P('phase', 'enc', 'pat'), parts along dimension 2, may hold values 0 or 1
Outputs:
- image_estimate: float32 [4, 4, 4, 4, 64, 192], P('pat', 'phase', 'enc', None, 'slab'), parts along dimension 0
- residual: float32 [4, 4, 4, 96, 64, 192], P('pat', 'phase', 'enc', 'slab'), parts along dimension 0
The draws below stay inside these ranges and needn't reach their ends.
There are 2 independent parts, one for each index of `pat`. The reference program is written for one: setup_inputs(seed, part) draws one part's arguments, and reference() takes and returns one part's arrays. A program takes and returns all parts, laid end to end along the dimension named above; each array names one. Nothing has to cross between parts.
All inputs are finite; a program needn't handle non-finite values. No bound on the sum of `sampling` on one device may be relied on, other than what follows from the above.
Results may differ from the reference program's by a relative error of at most 0.0046.
Values may be sent and summed in bfloat16 or wider, within the bound.
No kernel may reach another device: no remote copies, remote signals or barrier semaphores. Data moves between devices by JAX's collectives and lax.ppermute only.
A program may use at most 64 MiB of HBM per device.

```python
import math
import jax
import jax.numpy as jnp
from jax import lax

NY = 192
NZ = 64
COILS = 24
ENC = 4
NXW = 4
ITERS = 2
PHASES = 4
ROWS = 96


def draw_coil_maps(key, part):
    shape = (2, COILS, NXW, NZ, NY)
    coil_level = 1.0 + 2.0 * jnp.arange(COILS, dtype=jnp.float32) / max(COILS - 1, 1)
    depth_level = 1.0 + 2.0 * jnp.arange(NZ, dtype=jnp.float32) / max(NZ - 1, 1)
    envelope = jnp.sqrt(coil_level[:, None, None, None] * depth_level[None, None, :, None])
    entries = jax.random.normal(key, shape, jnp.float32)
    values = entries * envelope[None] / jnp.sqrt(8.0 * COILS)
    return jnp.clip(values, -1.0, 1.0).astype(jnp.bfloat16)


def plant(values, own_key, low, largest):
    longest = values.shape.index(max(values.shape))
    spots = []
    for shift in (0, 1):
        where = [jax.random.randint(jax.random.fold_in(own_key, axis), (), 0, length) for axis, length in enumerate(values.shape)]
        where[longest] = (where[longest] + shift) % values.shape[longest]
        spots.append(tuple(where))
    return values.at[spots[0]].set(low).at[spots[1]].set(largest)


def level_of(rng, dims, cuts, least, top_value):
    def one(dim, shards_of):
        steps = jax.random.uniform(jax.random.fold_in(jax.random.fold_in(rng, 6), dim), (shards_of,), jnp.float32, least / len(cuts), top_value / len(cuts))
        return jnp.repeat(jnp.exp(steps), dims[dim] // shards_of).reshape((-1,) + (1,) * (len(dims) - dim - 1))

    factor_of = one(*cuts[0])
    for cut in cuts[1:]:
        factor_of = factor_of * one(*cut)
    return factor_of


def centred(stream_key, dims, scale, most, shards=(), held_as=jnp.bfloat16):
    loudness = level_of(stream_key, dims, shards, -0.22, 0.18) if shards else 1.0
    drawn = jax.random.normal(stream_key, dims, jnp.float32) * scale * loudness
    return jnp.minimum(jnp.maximum(drawn, -most), most).astype(held_as)


def setup_inputs(seed: int = 0, part: int = 0) -> dict:
    key_list = jax.random.split(jax.random.key(seed), 4)
    part_splits = jax.random.split(jax.random.fold_in(key_list[3], part), 4)
    kspace_data = centred(part_splits[0], (2, PHASES, ENC, ROWS, NZ, NY), 1.0, 6.0, ((1, 4), (2, 2), (3, 32)))
    coil_maps = draw_coil_maps(jax.random.fold_in(jax.random.fold_in(key_list[3], part), 71), part)
    sampling = plant((jax.random.randint(part_splits[2], (PHASES, ENC, NZ, NY), 0, 3) < 1).astype(jnp.int32), jax.random.fold_in(part_splits[2], 1), 0, 1)
    return dict(kspace_data=kspace_data, coil_maps=coil_maps, sampling=sampling)


tv_weight = 0.15
smoothing = 0.6

def dft_table(length, direction):
    counter = jnp.arange(length, dtype=jnp.int32)
    product = counter[:, None] * counter[None, :] % length
    angle = product.astype(jnp.float32) * (2.0 * math.pi / length)
    factor = 1.0 / math.sqrt(length)
    return ((jnp.cos(angle) * factor).astype(jnp.bfloat16), (direction * jnp.sin(angle) * factor).astype(jnp.bfloat16))

def rounded(values):
    return lax.optimization_barrier(values.astype(jnp.bfloat16))

def along_rows(real_part, imag_part, table):
    cosine = table[0].astype(jnp.float32)
    sine = table[1].astype(jnp.float32)
    first = real_part.astype(jnp.float32)
    second = imag_part.astype(jnp.float32)
    real_out = jnp.einsum('...y,yw->...w', first, cosine) - jnp.einsum('...y,yw->...w', second, sine)
    imag_out = jnp.einsum('...y,yw->...w', first, sine) + jnp.einsum('...y,yw->...w', second, cosine)
    return (real_out, imag_out)

def along_depth(real_part, imag_part, table):
    cosine = table[0].astype(jnp.float32)
    sine = table[1].astype(jnp.float32)
    first = real_part.astype(jnp.float32)
    second = imag_part.astype(jnp.float32)
    real_out = jnp.einsum('...zy,zw->...wy', first, cosine) - jnp.einsum('...zy,zw->...wy', second, sine)
    imag_out = jnp.einsum('...zy,zw->...wy', first, sine) + jnp.einsum('...zy,zw->...wy', second, cosine)
    return (real_out, imag_out)

def forward_phase(values, sampled_phase, coil_maps, tables):
    base = rounded(values).astype(jnp.float32)
    coil_real = coil_maps[0].astype(jnp.float32)
    coil_imag = coil_maps[1].astype(jnp.float32)
    real_in = base[0][:, None]
    imag_in = base[1][:, None]
    prod_real = rounded(coil_real * real_in - coil_imag * imag_in)
    prod_imag = rounded(coil_real * imag_in + coil_imag * real_in)
    mid_real, mid_imag = along_rows(prod_real, prod_imag, tables[0])
    mid_real = rounded(mid_real).reshape(ENC, ROWS, NZ, NY)
    mid_imag = rounded(mid_imag).reshape(ENC, ROWS, NZ, NY)
    out_real, out_imag = along_depth(mid_real, mid_imag, tables[1])
    weight = sampled_phase[:, None]
    return jnp.stack([out_real * weight, out_imag * weight])

def adjoint_phase(values, coil_maps, tables):
    low_real = rounded(values[0])
    low_imag = rounded(values[1])
    mid_real, mid_imag = along_depth(low_real, low_imag, tables[3])
    mid_real = rounded(mid_real).reshape(ENC, COILS, NXW, NZ, NY)
    mid_imag = rounded(mid_imag).reshape(ENC, COILS, NXW, NZ, NY)
    coil_real = coil_maps[0].astype(jnp.float32)
    coil_imag = coil_maps[1].astype(jnp.float32)
    fine_real, fine_imag = along_rows(mid_real, mid_imag, tables[2])
    grad_real = lax.optimization_barrier(jnp.sum(coil_real * fine_real + coil_imag * fine_imag, axis=1))
    grad_imag = lax.optimization_barrier(jnp.sum(coil_real * fine_imag - coil_imag * fine_real, axis=1))
    return jnp.stack([grad_real, grad_imag])

def total_variation(values):
    difference = jnp.roll(values, -1, axis=1) - values
    modulus = difference[0] * difference[0] + difference[1] * difference[1]
    weights = difference / jnp.sqrt(modulus + smoothing * smoothing)[None]
    return jnp.roll(weights, 1, axis=1) - weights

def reference(kspace_data, coil_maps, sampling):
    tables = (dft_table(NY, -1.0), dft_table(NZ, -1.0), dft_table(NY, 1.0), dft_table(NZ, 1.0))
    sampled = sampling.astype(jnp.float32)
    residual = -(kspace_data.astype(jnp.float32) * sampled[None, :, :, None])
    image_estimate = jnp.zeros((2, PHASES, ENC, NXW, NZ, NY), jnp.float32)
    for iteration in range(ITERS):
        moved = jnp.moveaxis(residual, 1, 0)
        adjoint = lax.map(lambda values: adjoint_phase(values, coil_maps, tables), moved)
        gradient = jnp.moveaxis(adjoint, 0, 1) + tv_weight * total_variation(image_estimate)
        grad_sq = jnp.sum(gradient * gradient)
        moved_grad = jnp.moveaxis(gradient, 1, 0)
        spectrum = lax.map(lambda pair: forward_phase(pair[0], pair[1], coil_maps, tables), (moved_grad, sampled))
        spectrum = jnp.moveaxis(spectrum, 0, 1)
        spec_sq = jnp.sum(spectrum * spectrum)
        alpha = grad_sq / (spec_sq + 4.0 * tv_weight / smoothing * grad_sq + 1e-06)
        image_estimate = image_estimate - alpha * gradient
        residual = residual - alpha * spectrum
    return (image_estimate, residual)
```

```python
import functools
import math

import jax
import jax.numpy as jnp
from jax import lax
from jax.experimental import pallas as pl
from jax.experimental.pallas import tpu as pltpu
from jax.sharding import Mesh
from jax.sharding import PartitionSpec as P

tv_weight = 0.15
smoothing = 0.6


def dft_table(length, direction):
    counter = jnp.arange(length, dtype=jnp.int32)
    product = counter[:, None] * counter[None, :] % length
    angle = product.astype(jnp.float32) * (2.0 * math.pi / length)
    factor = 1.0 / math.sqrt(length)
    return (
        (jnp.cos(angle) * factor).astype(jnp.bfloat16),
        (direction * jnp.sin(angle) * factor).astype(jnp.bfloat16),
    )


def depth_block(length, direction):
    cosine, sine = dft_table(length, direction)
    top = jnp.concatenate([cosine, -sine], axis=1)
    bottom = jnp.concatenate([sine, cosine], axis=1)
    return jnp.concatenate([top, bottom], axis=0)


def dot(a, b):
    return jnp.dot(a, b, preferred_element_type=jnp.float32)


def along_rows(real_part, imag_part, table):
    cosine, sine = table
    return (
        dot(real_part, cosine) - dot(imag_part, sine),
        dot(real_part, sine) + dot(imag_part, cosine),
    )


def adjoint_start(kspace_data, sampled, depth_inv):
    encodings, rows, slices, lines = kspace_data.shape[1:]

    def kernel(data, mask, table, out):
        for e in range(encodings):
            weight = -mask[e].astype(jnp.float32)
            for r in range(rows):
                real = (data[0, e, r].astype(jnp.float32) * weight).astype(jnp.bfloat16)
                imag = (data[1, e, r].astype(jnp.float32) * weight).astype(jnp.bfloat16)
                both = dot(table[...], jnp.concatenate([real, imag], axis=0)).astype(jnp.bfloat16)
                out[0, e, r] = both[:slices]
                out[1, e, r] = both[slices:]

    return pl.pallas_call(
        kernel, out_shape=jax.ShapeDtypeStruct(kspace_data.shape, jnp.bfloat16), name="adjoint_start"
    )(kspace_data, sampled, depth_inv)


def normal_step(where, image, extra, sampled, coils_own, coils_other, tables, second):
    column_fwd, column_inv, depth_fwd, depth_inv = tables
    _, encodings, slices, lines = image.shape
    steps, _, group = coils_own.shape[:3]
    nlo = 4
    padded = slices + 16
    f32 = jnp.float32
    bf16 = jnp.bfloat16

    def kernel(*refs):
        refs = list(refs)
        where_ref = refs.pop(0)
        if second:
            alpha_ref = refs.pop(0)
            image_ref, before_ref, after_ref, normal_ref = (refs.pop(0) for _ in range(4))
        else:
            image_ref = refs.pop(0)
        mask_ref, own_ref, other_ref = (refs.pop(0) for _ in range(3))
        fc, fs, ic, isn, zf, zi = (refs.pop(0) for _ in range(6))
        send_ref, norm_ref = refs.pop(0), refs.pop(0)
        if not second:
            out_ref = refs.pop(0)
        value, masked, ee, gg = refs
        step = pl.program_id(0)
        hi, lo, core = where_ref[0], where_ref[1], where_ref[2]

        @pl.when(step == 0)
        def _():
            total = jnp.zeros((slices, lines), f32)
            for e in range(encodings):
                if second:
                    alpha = alpha_ref[0]
                    now = [-alpha * image_ref[c, e].astype(f32) for c in range(2)]
                    back = [-alpha * before_ref[c, e].astype(f32) for c in range(2)]
                    ahead = [-alpha * after_ref[c, e].astype(f32) for c in range(2)]
                    d0 = [now[c] - back[c] for c in range(2)]
                    d1 = [ahead[c] - now[c] for c in range(2)]
                    s0 = jnp.sqrt(d0[0] * d0[0] + d0[1] * d0[1] + smoothing * smoothing)
                    s1 = jnp.sqrt(d1[0] * d1[0] + d1[1] * d1[1] + smoothing * smoothing)
                    new = [
                        image_ref[c, e].astype(f32)
                        - alpha * normal_ref[c, e]
                        + tv_weight * (d0[c] / s0 - d1[c] / s1)
                        for c in range(2)
                    ]
                else:
                    new = [image_ref[c, e].astype(f32) for c in range(2)]
                for c in range(2):
                    value[c, e] = new[c]
                    total = total + new[c] * new[c]
            gg[...] = total
            ee[...] = jnp.zeros((slices, lines), f32)
            if not second:
                out_ref[...] = jnp.zeros(out_ref.shape, f32)

        for half, coil_ref in ((0, own_ref), (1, other_ref)):
            for k in range(group):
                coil_real = coil_ref[0, 0, k].astype(f32)
                coil_imag = coil_ref[0, 1, k].astype(f32)
                for e in range(encodings):
                    real = value[0, e].astype(bf16).astype(f32)
                    imag = value[1, e].astype(bf16).astype(f32)
                    a = (coil_real * real - coil_imag * imag).astype(bf16)
                    b = (coil_real * imag + coil_imag * real).astype(bf16)
                    u_real, u_imag = along_rows(a, b, (fc[...], fs[...]))
                    both = jnp.concatenate([u_real.astype(bf16), u_imag.astype(bf16)], axis=0)
                    spectrum = dot(zf[...], both)
                    weight = mask_ref[e].astype(f32)
                    s_real = spectrum[:slices] * weight
                    s_imag = spectrum[slices:] * weight
                    ee[...] += s_real * s_real + s_imag * s_imag
                    low_real, low_imag = s_real.astype(bf16), s_imag.astype(bf16)
                    masked[half, k, 0, e] = low_real
                    masked[half, k, 1, e] = low_imag
                    if not second:
                        p = dot(zi[...], jnp.concatenate([low_real, low_imag], axis=0)).astype(bf16)
                        q_real, q_imag = along_rows(p[:slices], p[slices:], (ic[...], isn[...]))
                        out_ref[0, e] += coil_real * q_real + coil_imag * q_imag
                        out_ref[1, e] += coil_real * q_imag - coil_imag * q_real
            owner = 2 * step + (core if half == 0 else 1 - core)

            @pl.when(owner == hi)
            def _():
                for dest in range(nlo):
                    i = lax.rem(lo + dest, nlo)
                    coil = jnp.minimum((3 * dest + i) // nlo, group - 1)
                    send_ref[dest, :, :, :slices] = masked[half, coil]

        @pl.when(step == steps - 1)
        def _():
            if second:
                for c in range(2):
                    for e in range(encodings):
                        piece = value[c, e, pl.ds(pl.multiple_of(8 * hi, 8), 8), :]
                        piece = jnp.concatenate([piece, jnp.zeros((8, lines), f32)], axis=0).astype(bf16)
                        for dest in range(nlo):
                            send_ref[dest, c, e, slices : slices + 16] = piece
            norm_ref[0] = jnp.sum(gg[...])
            norm_ref[1] = jnp.sum(ee[...])

    def whole(array):
        return pl.BlockSpec(array.shape, lambda g, _n=array.ndim: (0,) * _n)

    smem = pl.BlockSpec(memory_space=pltpu.SMEM)
    arrays = [image, *extra[1:], sampled]
    consts = [*column_fwd, *column_inv, depth_fwd, depth_inv]
    coil_spec = pl.BlockSpec((1,) + coils_own.shape[1:], lambda g: (g, 0, 0, 0, 0))
    operands = [where] + ([extra[0]] if second else []) + arrays + [coils_own, coils_other] + consts
    in_specs = (
        [smem]
        + ([smem] if second else [])
        + [whole(a) for a in arrays]
        + [coil_spec, coil_spec]
        + [whole(a) for a in consts]
    )
    send = jax.ShapeDtypeStruct((nlo, 2, encodings, padded if second else slices, lines), bf16)
    outs = [send, jax.ShapeDtypeStruct((2,), f32)]
    out_specs = [whole(send), smem]
    if not second:
        outs.append(jax.ShapeDtypeStruct(image.shape, f32))
        out_specs.append(whole(outs[-1]))
    return pl.pallas_call(
        kernel,
        grid=(steps,),
        in_specs=in_specs,
        out_specs=out_specs,
        out_shape=outs,
        scratch_shapes=[
            pltpu.VMEM(image.shape, f32),
            pltpu.VMEM((2, group, 2, encodings, slices, lines), bf16),
            pltpu.VMEM((slices, lines), f32),
            pltpu.VMEM((slices, lines), f32),
        ],
        name="second_step" if second else "first_step",
    )(*operands)


def finish(where, alphas, kspace_data, sampled, rows_one, rows_two):
    encodings, rows, slices, lines = kspace_data.shape[1:]
    nlo = 4

    def kernel(where_ref, alpha, data, mask, one, two, out):
        lo = where_ref[1]
        for r in range(rows):
            source = lax.rem(r - lo + nlo, nlo)
            for e in range(encodings):
                weight = mask[e].astype(jnp.float32)
                for c in range(2):
                    start = -(data[c, e, r].astype(jnp.float32) * weight)
                    first = one[source, c, e].astype(jnp.float32)
                    last = two[source, c, e, :slices].astype(jnp.float32)
                    out[c, e, r] = start - alpha[0] * first - alpha[1] * last

    smem = pl.BlockSpec(memory_space=pltpu.SMEM)
    vmem = pl.BlockSpec(memory_space=pltpu.VMEM)
    return pl.pallas_call(
        kernel,
        in_specs=[smem, smem, vmem, vmem, vmem, vmem],
        out_specs=vmem,
        out_shape=jax.ShapeDtypeStruct(kspace_data.shape, jnp.float32),
        name="finish",
    )(where, alphas, kspace_data, sampled, rows_one, rows_two)


def body(kspace_data, coil_maps, sampling):
    encodings = kspace_data.shape[2]
    rows = kspace_data.shape[3]
    slices = kspace_data.shape[4]
    coils, readout, zdepth, lines = coil_maps.shape[1:]
    nhi, nlo = lax.axis_size("hi"), lax.axis_size("lo")
    nphase, ncore = lax.axis_size("phase"), lax.axis_size("enc")
    slabs = nhi * nlo
    group = coils // (nphase * ncore)
    hi, lo = lax.axis_index("hi"), lax.axis_index("lo")
    phase, core = lax.axis_index("phase"), lax.axis_index("enc")
    where = jnp.stack([hi, lo, core]).astype(jnp.int32)
    column_fwd = dft_table(lines, -1.0)
    column_inv = dft_table(lines, 1.0)
    depth_fwd = depth_block(slices, -1.0)
    depth_inv = depth_block(slices, 1.0)
    tables = (column_fwd, column_inv, depth_fwd, depth_inv)
    sampled = sampling[0].astype(jnp.float32)
    data = kspace_data[:, 0]

    start = adjoint_start(data, sampled, depth_inv)
    start = start.reshape(2, encodings, rows, slabs, zdepth, lines)
    start = start.transpose(3, 0, 1, 2, 4, 5).reshape(slabs, 4 * rows * zdepth, lines)
    share = lax.dynamic_slice_in_dim(coil_maps, (phase * ncore + core) * group, group, axis=1)
    share = share.transpose(2, 0, 1, 3, 4).reshape(1, readout, 2 * group * zdepth, lines)
    share = jnp.broadcast_to(share, (nhi,) + share.shape[1:]).reshape(slabs, -1, lines)
    packed = jnp.concatenate([start, share], axis=1)
    packed = lax.all_to_all(packed, ("hi", "lo"), 0, 0, tiled=True)
    part = packed[:, : start.shape[1]].reshape(slabs, 2, encodings, rows, zdepth, lines)
    part = part.transpose(1, 2, 0, 3, 4, 5).reshape(2, encodings, coils, readout, zdepth, lines)
    share = packed[:, start.shape[1] :].reshape(slabs, 2, group, zdepth, lines)
    share = share.transpose(1, 2, 0, 3, 4).reshape(2, group, slices, lines)

    coil_real = coil_maps[0].astype(jnp.float32)
    coil_imag = coil_maps[1].astype(jnp.float32)
    fine_real = dot(part[0], column_inv[0]) - dot(part[1], column_inv[1])
    fine_imag = dot(part[0], column_inv[1]) + dot(part[1], column_inv[0])
    grad_real = jnp.sum(coil_real * fine_real + coil_imag * fine_imag, axis=1)
    grad_imag = jnp.sum(coil_real * fine_imag - coil_imag * fine_real, axis=1)
    slab_one = jnp.stack([grad_real, grad_imag])

    spread = slab_one.transpose(2, 0, 1, 3, 4)[None].astype(GRAD)
    spread = jnp.broadcast_to(spread, (nhi,) + spread.shape[1:]).reshape(slabs, *spread.shape[2:])
    spread = lax.all_to_all(spread, ("hi", "lo"), 0, 0, tiled=True)
    one = spread.transpose(1, 2, 0, 3, 4).reshape(2, encodings, slices, lines)

    own = lax.all_gather(share, "phase")
    other = lax.ppermute(own, "enc", [(i, (i + 1) % ncore) for i in range(ncore)])

    up = [(i, (i + 1) % nphase) for i in range(nphase)]
    before = lax.ppermute(one, "phase", up)
    after = lax.ppermute(one, "phase", [(j, i) for i, j in up])

    def total(norms):
        norms = functools.reduce(lax.psum, ("lo", "phase", "enc"), norms)
        return norms[0] / (norms[1] + 4.0 * tv_weight / smoothing * norms[0] + 1e-06)

    send_one, norms, normal = normal_step(where, one, (), sampled, own, other, tables, False)
    rows_one = lax.all_to_all(send_one, "lo", 0, 0, tiled=True)
    alpha_one = total(norms)
    extra = (alpha_one.reshape(1), before, after, normal)
    send_two, norms = normal_step(where, one, extra, sampled, own, other, tables, True)
    rows_two = lax.all_to_all(send_two, "lo", 0, 0, tiled=True)
    alpha_two = total(norms)

    slab_two = lax.dynamic_slice_in_dim(rows_two, slices + zdepth * lo, zdepth, axis=3)
    slab_two = slab_two.transpose(1, 2, 0, 3, 4).astype(jnp.float32)
    image = -alpha_one * slab_one - alpha_two * slab_two
    alphas = jnp.stack([alpha_one, alpha_two])
    residual = finish(where, alphas, data, sampled, rows_one, rows_two)
    return (image[:, None], residual[:, None])


GRAD = jnp.bfloat16


def solution(mesh):
    names = dict(mesh.shape)
    nlo = 4
    grid = Mesh(
        mesh.devices.reshape(names["pat"], names["slab"] // nlo, nlo, names["phase"], names["enc"]),
        ("pat", "hi", "lo", "phase", "enc"),
    )
    slab = ("hi", "lo")
    in_specs = (
        P("pat", "phase", "enc", slab, None, None),
        P("pat", None, None, slab, None),
        P("phase", "enc", "pat", None),
    )
    out_specs = (
        P("pat", "phase", "enc", None, slab, None),
        P("pat", "phase", "enc", slab, None, None),
    )
    return jax.shard_map(body, mesh=grid, in_specs=in_specs, out_specs=out_specs, check_vma=False)
```

```python
import math

import jax
import jax.numpy as jnp
import numpy as np
from jax import lax
from jax.experimental import pallas as pl
from jax.experimental.pallas import tpu as pltpu
from jax.sharding import Mesh
from jax.sharding import PartitionSpec as P

tv_weight = 0.15
smoothing = 0.6
f32 = jnp.float32
bf16 = jnp.bfloat16

LANE = 128
HALF = 64
WIDE = 384


def dft(length, direction):
    counter = np.arange(length)
    angle = (counter[:, None] * counter[None, :] % length).astype(np.float32) * np.float32(2.0 * math.pi / length)
    factor = np.float32(1.0 / math.sqrt(length))
    return np.cos(angle) * factor, np.float32(direction) * np.sin(angle) * factor


def column_table(length, direction):
    real, imag = dft(length, direction)
    whole = np.concatenate(
        [np.concatenate([real, imag], axis=1), np.concatenate([-imag, real], axis=1)], axis=0
    )
    order = np.concatenate(
        [
            np.arange(LANE),
            length + np.arange(LANE),
            np.arange(LANE, length),
            length + np.arange(LANE, length),
        ]
    )
    packed = whole[order][:, order]
    tail = np.concatenate([-packed[:, WIDE - HALF :], packed[:, WIDE - LANE : WIDE - HALF]], axis=1)
    return jnp.asarray(np.concatenate([packed, tail], axis=1), dtype=bf16)


def depth_table(length, direction):
    real, imag = dft(length, direction)
    return jnp.asarray(
        np.concatenate(
            [np.concatenate([real, -imag], axis=1), np.concatenate([imag, real], axis=1)], axis=0
        ),
        dtype=bf16,
    )


def dot(a, b):
    return jnp.dot(a, b, preferred_element_type=f32)


def lanes(*pieces):
    return jnp.concatenate(pieces, axis=1)


def stack(*pieces):
    return jnp.concatenate(pieces, axis=0)


def left_half(shape):
    return lax.broadcasted_iota(jnp.int32, shape, 1) < HALF


def swapped(d):
    return pltpu.roll(d, HALF, 1)


def times_i(d):
    other = swapped(d)
    return jnp.where(left_half(d.shape), -other, other)


def doubled(d):
    other = swapped(d)
    left = left_half(d.shape)
    return jnp.where(left, d, other), jnp.where(left, other, d)


def mask_lanes(mask):
    mask = mask.astype(f32)
    return mask[:, :LANE], lanes(mask[:, LANE:], mask[:, LANE:])


def call(kernel, name, flops, **kwargs):
    return pl.pallas_call(
        kernel,
        name=name,
        cost_estimate=pl.CostEstimate(flops=flops, transcendentals=0, bytes_accessed=2**20),
        **kwargs,
    )


SMEM = pl.BlockSpec(memory_space=pltpu.SMEM)
VMEM = pl.BlockSpec(memory_space=pltpu.VMEM)


def depart(where, data, sampling, coils, depth_inv, nhi, group):
    encodings, rows, slices, _ = data.shape[1:]
    images = encodings * rows

    def kernel(where_ref, data_ref, mask_ref, coil_ref, table, out):
        for e in range(encodings):
            weight = -mask_ref[e].astype(f32)
            for r in range(rows):
                both = stack(*((data_ref[c, e, r].astype(f32) * weight).astype(bf16) for c in range(2)))
                both = dot(table[...], both)
                real, imag = both[:slices], both[slices:]
                at = (e * rows + r) * WIDE
                out[:, at : at + LANE] = real[:, :LANE].astype(bf16)
                out[:, at + LANE : at + 2 * LANE] = imag[:, :LANE].astype(bf16)
                out[:, at + 2 * LANE : at + WIDE] = lanes(real[:, LANE:], imag[:, LANE:]).astype(bf16)
        first = where_ref[3] * group
        for k in range(group):
            real, imag = coil_ref[0, first + k].astype(f32), coil_ref[1, first + k].astype(f32)
            block = lanes(real[:, :LANE], imag[:, :LANE], lanes(real[:, LANE:], imag[:, LANE:]))
            block = stack(block, block).astype(bf16)
            at = (images + k) * WIDE
            for h in range(nhi // 2):
                out[16 * h : 16 * h + 16, at : at + WIDE] = block

    return call(
        kernel,
        "depart",
        10**8,
        in_specs=[SMEM, VMEM, VMEM, VMEM, VMEM],
        out_specs=VMEM,
        out_shape=jax.ShapeDtypeStruct((slices, (images + group) * WIDE), bf16),
    )(where, data, sampling, coils, depth_inv)


def slab_gradient(packed, coil_rows, column_inv, encodings, nhi):
    rows, _, slices, lines = coil_rows.shape

    def kernel(in_ref, coil_ref, table, out, send):
        images = [in_ref[:, i * WIDE : (i + 1) * WIDE] for i in range(encodings * rows)]
        fine = dot(stack(*images), table[...])
        coil = []
        for r in range(rows):
            real, imag = coil_ref[r, 0].astype(f32), coil_ref[r, 1].astype(f32)
            coil.append(
                (
                    real[:, :LANE],
                    imag[:, :LANE],
                    lanes(real[:, LANE:], real[:, LANE:]),
                    lanes(imag[:, LANE:], imag[:, LANE:]),
                )
            )
        even = lax.rem(lax.broadcasted_iota(jnp.int32, (8, WIDE), 0) // 2, 2) == 0
        for e in range(encodings):
            total = jnp.zeros((8, WIDE), f32)
            for r in range(rows):
                at = (e * rows + r) * slices
                a, b, d, t = (fine[at : at + slices, j * LANE : (j + 1) * LANE] for j in range(4))
                ca, cb, dr, di = coil[r]
                value = lanes(ca * a + cb * b, ca * b - cb * a, dr * d - di * t)
                value = jnp.sum(value.reshape(slices // 8, 8, WIDE), axis=0)
                turned = (-2 * r) % 8
                one = value if turned == 0 else pltpu.roll(value, turned, 0)
                two = pltpu.roll(value, (turned + 4) % 8, 0) if (turned + 4) % 8 else value
                total = total + jnp.where(even, one, two)
            for x in range(4):
                out[x, :, e * WIDE : (e + 1) * WIDE] = pltpu.roll(total, 8 - 2 * x, 0) if x else total
            block = stack(total, total).astype(bf16)
            for h in range(nhi // 2):
                send[16 * h : 16 * h + 16, e * WIDE : (e + 1) * WIDE] = block

    return call(
        kernel,
        "slab_gradient",
        10**8,
        in_specs=[VMEM, VMEM, VMEM],
        out_specs=[VMEM, VMEM],
        out_shape=[
            jax.ShapeDtypeStruct((4, 8, encodings * WIDE), f32),
            jax.ShapeDtypeStruct((slices, encodings * WIDE), bf16),
        ],
    )(packed, coil_rows, column_inv)


def step_length(norm_ref):
    gg, ee = (jnp.sum(norm_ref[:, i : i + 1, :], axis=0) for i in range(2))
    return gg / (ee + 4.0 * tv_weight / smoothing * gg + 1e-06)


def image_step(where, image, extra, sampling, own, other, tables, nlo, members, second):
    column_fwd, column_inv, depth_fwd, depth_inv = tables
    slices, width = image.shape
    encodings = width // WIDE
    steps = own.shape[0]
    group = own.shape[2] // WIDE
    block = group * encodings * slices

    def kernel(*refs):
        refs = list(refs)
        where_ref = refs.pop(0)
        if second:
            norms_ref, image_ref, before_ref, after_ref, normal_ref, *firsts = (refs.pop(0) for _ in range(8))
        else:
            image_ref = refs.pop(0)
        mask_ref, own_ref, other_ref, wf, wi, zf, zi = (refs.pop(0) for _ in range(7))
        sends = [refs.pop(0) for _ in range(3)]
        norm_ref, out_ref = refs.pop(0), refs.pop(0)
        value, ahead_ref, mask_a, mask_d, masked, product, squares = refs
        step = pl.program_id(0)
        hi, lo, core = where_ref[0], where_ref[1], where_ref[2]

        def column(ref, e, j):
            at = e * WIDE + j * LANE
            return ref[:, at : at + LANE].astype(f32)

        @pl.when(step == 0)
        def _():
            total = jnp.zeros((slices, LANE), f32)
            for e in range(encodings):
                now = [column(image_ref, e, j) for j in range(3)]
                if second:
                    alpha = step_length(norms_ref)
                    new = [-alpha * v for v in now]
                    slopes = []
                    for d in (
                        [new[j] + alpha * column(before_ref, e, j) for j in range(3)],
                        [-alpha * column(after_ref, e, j) - new[j] for j in range(3)],
                    ):
                        near = jnp.sqrt(d[0] * d[0] + d[1] * d[1] + smoothing * smoothing)
                        square = d[2] * d[2]
                        far = jnp.sqrt(square + swapped(square) + smoothing * smoothing)
                        slopes.append([d[0] / near, d[1] / near, d[2] / far])
                    now = [
                        now[j] - alpha * column(normal_ref, e, j) + tv_weight * (slopes[0][j] - slopes[1][j])
                        for j in range(3)
                    ]
                    for j in range(3):
                        at = e * WIDE + j * LANE
                        ahead_ref[:, at : at + LANE] = now[j]
                for j in range(3):
                    at = e * WIDE + j * LANE
                    total = total + now[j] * now[j]
                    now[j] = now[j].astype(bf16).astype(f32)
                    value[:, e * 512 + j * LANE : e * 512 + (j + 1) * LANE] = now[j]
                value[:, e * 512 + 3 * LANE : (e + 1) * 512] = times_i(now[2])
                a, d = mask_lanes(mask_ref[e])
                mask_a[:, e * LANE : (e + 1) * LANE] = a
                mask_d[:, e * LANE : (e + 1) * LANE] = d
            norm_ref[:, 0:1, :] = jnp.full((members, 1, LANE), jnp.sum(total), f32)
            squares[...] = jnp.zeros(squares.shape, f32)
            if not second:
                out_ref[...] = jnp.zeros(out_ref.shape, f32)

        for half, coil_ref in ((0, own_ref), (1, other_ref)):

            def coil_lanes(k):
                a, b, d = (coil_ref[0, :, k * WIDE + j * LANE : k * WIDE + (j + 1) * LANE].astype(f32) for j in range(3))
                return (a, b, *doubled(d))

            for k in range(group):
                ca, cb, dr, di = coil_lanes(k)
                for e in range(encodings):
                    va, vb, vd, vt = (value[:, e * 512 + j * LANE : e * 512 + (j + 1) * LANE] for j in range(4))
                    at = (k * encodings + e) * slices
                    product[at : at + slices, :LANE] = (ca * va - cb * vb).astype(bf16)
                    product[at : at + slices, LANE : 2 * LANE] = (ca * vb + cb * va).astype(bf16)
                    product[at : at + slices, 2 * LANE :] = (dr * vd + di * vt).astype(bf16)
            u = dot(product[...], wf[...]).astype(bf16)
            weight_a, weight_d = mask_a[...], mask_d[...]
            total = jnp.zeros(weight_a.shape, f32)
            for k in range(group):

                def pair(j):
                    return lanes(
                        *(
                            u[(k * encodings + e) * slices : (k * encodings + e + 1) * slices, j * LANE : (j + 1) * LANE]
                            for e in range(encodings)
                        )
                    )

                near = dot(zf[...], stack(pair(0), pair(1)))
                far = dot(zi[...], stack(pair(2), pair(3)))
                sa, sb = near[:slices] * weight_a, near[slices:] * weight_a
                sd, st = far[:slices] * weight_d, far[slices:] * weight_d
                total = total + (sa * sa + sb * sb + sd * sd)
                sa, sb, sd, st = (x.astype(bf16) for x in (sa, sb, sd, st))
                for e in range(encodings):
                    for j, x in enumerate((sa, sb, sd)):
                        at = e * WIDE + j * LANE
                        masked[half * group + k, :, at : at + LANE] = x[:, e * LANE : (e + 1) * LANE]
                if not second:
                    near = dot(zi[...], stack(sa, sb)).astype(bf16)
                    far = dot(zf[:slices, :], stack(sd, st)).astype(bf16)
                    for e in range(encodings):
                        at = (k * encodings + e) * slices
                        for j, x in enumerate((near[:slices], near[slices:], far)):
                            product[at : at + slices, j * LANE : (j + 1) * LANE] = x[:, e * LANE : (e + 1) * LANE]
            squares[...] += total
            if not second:
                q = dot(product[...], wi[...])
                sums = [[0.0, 0.0, 0.0] for _ in range(encodings)]
                for k in range(group):
                    ca, cb, dr, di = coil_lanes(k)
                    for e in range(encodings):
                        at = (k * encodings + e) * slices
                        qa, qb, qd, qt = (q[at : at + slices, j * LANE : (j + 1) * LANE] for j in range(4))
                        sums[e][0] += ca * qa + cb * qb
                        sums[e][1] += ca * qb - cb * qa
                        sums[e][2] += dr * qd - di * qt
                for e in range(encodings):
                    for j in range(3):
                        at = e * WIDE + j * LANE
                        out_ref[:, at : at + LANE] += sums[e][j]
            owner = 2 * step + (core if half == 0 else 1 - core)

            @pl.when(owner == hi)
            def _():
                for j, send_ref in enumerate(sends):
                    dest = lax.bitwise_xor(lo, j)
                    coil = (3 * dest + lax.rem(lo + dest, nlo)) // nlo
                    send_ref[:slices] = masked[half * group + coil]

        @pl.when(step == steps - 1)
        def _():
            if second:
                piece = ahead_ref[pl.ds(pl.multiple_of(8 * hi, 8), 8), :]
                turned = [pltpu.roll(piece, 8 - 2 * dest, 0) if dest else piece for dest in range(nlo)]
                for j in range(nlo):
                    dest = lax.bitwise_xor(lo, j)
                    part = turned[0]
                    for k in range(1, nlo):
                        part = jnp.where(dest == k, turned[k], part)
                    part = stack(part, part).astype(bf16)
                    if j < 3:
                        sends[j][slices : slices + 16] = part
                        sends[j][slices + 16 :] = firsts[j][...]
                    else:
                        out_ref[...] = part
            norm_ref[:, 1:2, :] = jnp.full((members, 1, LANE), jnp.sum(squares[...]), f32)

    def whole(array):
        return pl.BlockSpec(array.shape, lambda g, _n=array.ndim: (0,) * _n)

    coil_spec = pl.BlockSpec((1,) + own.shape[1:], lambda g: (g, 0, 0))
    consts = [column_fwd, column_inv, depth_fwd, depth_inv]
    arrays = [*extra[:1], image, *extra[1:], sampling]
    height = 2 * slices + 16 if second else slices
    outs = [jax.ShapeDtypeStruct((height, width), bf16)] * 3
    outs.append(jax.ShapeDtypeStruct((members, 2, LANE), f32))
    outs.append(jax.ShapeDtypeStruct((16, width), bf16) if second else jax.ShapeDtypeStruct(image.shape, f32))
    return call(
        kernel,
        "second_step" if second else "first_step",
        (2 if second else 4) * 10**9,
        grid=(steps,),
        in_specs=[SMEM] + [whole(a) for a in arrays] + [coil_spec, coil_spec] + [whole(a) for a in consts],
        out_specs=[whole(o) for o in outs],
        out_shape=outs,
        scratch_shapes=[
            pltpu.VMEM((slices, encodings * 512), f32),
            pltpu.VMEM((slices, width), f32),
            pltpu.VMEM((slices, encodings * LANE), f32),
            pltpu.VMEM((slices, encodings * LANE), f32),
            pltpu.VMEM((2 * group, slices, width), bf16),
            pltpu.VMEM((block, WIDE), bf16),
            pltpu.VMEM((slices, encodings * LANE), f32),
        ],
    )(where, *arrays, own, other, *consts)


def finish(where, norms_one, norms_two, data, sampling, slab_one, rows, last, readout):
    encodings, nrows, slices, lines = data.shape[1:]

    def kernel(where_ref, norm_one, norm_two, data_ref, mask_ref, slab, keep, near, far, last_ref, out, image):
        lo = where_ref[1]
        alphas = step_length(norm_one), step_length(norm_two)
        for j, rows_ref in enumerate((keep, near, far)):
            r = jnp.where(lax.rem(lo, 2) == 0, j, nrows - 1 - j)
            for e in range(encodings):
                weight = mask_ref[e].astype(f32)
                real, imag = (-(data_ref[c, e, r].astype(f32) * weight) for c in range(2))
                a, b, d = (
                    alphas[0] * rows_ref[slices + 16 :, e * WIDE + k * LANE : e * WIDE + (k + 1) * LANE].astype(f32)
                    + alphas[1] * rows_ref[:slices, e * WIDE + k * LANE : e * WIDE + (k + 1) * LANE].astype(f32)
                    for k in range(3)
                )
                out[0, e, r, :, :LANE] = real[:, :LANE] - a
                out[1, e, r, :, :LANE] = imag[:, :LANE] - b
                out[0, e, r, :, LANE:] = real[:, LANE:] - d[:, :HALF]
                out[1, e, r, :, LANE:] = imag[:, LANE:] - swapped(d)[:, :HALF]
        for j in range(readout):
            x = lax.bitwise_xor(lo, j)
            for e in range(encodings):
                for k in range(3):
                    at = e * WIDE + k * LANE
                    if j < 3:
                        step = (keep, near, far)[j][slices : slices + 16, at : at + LANE]
                    else:
                        step = last_ref[:, at : at + LANE]
                    value = -alphas[0] * slab[x, :, at : at + LANE] - alphas[1] * step.astype(f32)[:8]
                    if k < 2:
                        image[k, e, x, :, :LANE] = value[:2]
                    else:
                        image[0, e, x, :, LANE:] = value[:2, :HALF]
                        image[1, e, x, :, LANE:] = swapped(value)[:2, :HALF]

    return call(
        kernel,
        "finish",
        10**7,
        in_specs=[SMEM] + [VMEM] * 9,
        out_specs=[VMEM, VMEM],
        out_shape=[
            jax.ShapeDtypeStruct(data.shape, f32),
            jax.ShapeDtypeStruct((2, encodings, readout, 2, lines), f32),
        ],
    )(where, norms_one, norms_two, data, sampling, slab_one, *rows, last)


def body(kspace_data, coil_maps, sampling):
    encodings = kspace_data.shape[2]
    rows = kspace_data.shape[3]
    slices = kspace_data.shape[4]
    coils, readout, zdepth, lines = coil_maps.shape[1:]
    nhi, nlo = lax.axis_size("hi"), lax.axis_size("lo")
    nphase, ncore = lax.axis_size("phase"), lax.axis_size("enc")
    slabs = nhi * nlo
    group = coils // (nphase * ncore)
    assert (nlo, readout, rows, zdepth, lines, slices) == (4, 4, 3, 2, LANE + HALF, 2 * slabs)
    assert group * nhi == coils and nphase * ncore == nhi and ncore == 2
    phase, core = lax.axis_index("phase"), lax.axis_index("enc")
    share_index = phase * ncore + core
    where = jnp.stack([lax.axis_index("hi"), lax.axis_index("lo"), core, share_index]).astype(jnp.int32)
    column_fwd, column_inv = column_table(lines, -1.0), column_table(lines, 1.0)
    depth_fwd, depth_inv = depth_table(slices, -1.0), depth_table(slices, 1.0)
    tables = (column_fwd, column_inv, depth_fwd, depth_inv)
    sampling = sampling[0]
    data = kspace_data[:, 0]

    def round_ring(value):
        value = value.reshape(slabs, zdepth, -1)
        return lax.all_to_all(value, ("hi", "lo"), 0, 0, tiled=True).reshape(slices, -1)

    packed = depart(where, data, sampling, coil_maps.reshape(2, coils, -1, lines), depth_inv, nhi, group)
    packed = round_ring(packed)
    coil_rows = coil_maps.reshape(2, slabs, rows, zdepth, lines).transpose(2, 0, 1, 3, 4)
    coil_rows = coil_rows.reshape(rows, 2, slices, lines)
    slab_one, spread = slab_gradient(packed, coil_rows, column_inv, encodings, nhi)
    one = round_ring(spread)
    own = lax.all_gather(packed[:, encodings * rows * WIDE :], "phase")
    other = lax.ppermute(own, "enc", [(i, (i + 1) % ncore) for i in range(ncore)])

    up = [(i, (i + 1) % nphase) for i in range(nphase)]
    before = lax.ppermute(one, "phase", up)
    after = lax.ppermute(one, "phase", [(j, i) for i, j in up])

    def total(norms):
        return lax.all_to_all(norms, ("lo", "phase", "enc"), 0, 0, tiled=True)

    members = nlo * nphase * ncore

    def swap(value, j):
        return lax.ppermute(value, "lo", [(i, i ^ j) for i in range(nlo)])

    *rows_one, norms, normal = image_step(where, one, (), sampling, own, other, tables, nlo, members, False)
    norms_one = total(norms)
    extra = (norms_one, before, after, normal, *rows_one)
    *rows_two, norms, last = image_step(where, one, extra, sampling, own, other, tables, nlo, members, True)
    norms_two = total(norms)
    got = [rows_two[0], swap(rows_two[1], 1), swap(rows_two[2], 2)]
    last = swap(last, 3)
    residual, image = finish(where, norms_one, norms_two, data, sampling, slab_one, got, last, readout)
    return (image[:, None], residual[:, None])


def solution(mesh):
    names = dict(mesh.shape)
    nlo = 4
    grid = Mesh(
        mesh.devices.reshape(names["pat"], names["slab"] // nlo, nlo, names["phase"], names["enc"]),
        ("pat", "hi", "lo", "phase", "enc"),
    )
    slab = ("hi", "lo")
    in_specs = (
        P("pat", "phase", "enc", slab, None, None),
        P("pat", None, None, slab, None),
        P("phase", "enc", "pat", None),
    )
    out_specs = (
        P("pat", "phase", "enc", None, slab, None),
        P("pat", "phase", "enc", slab, None, None),
    )
    return jax.shard_map(body, mesh=grid, in_specs=in_specs, out_specs=out_specs, check_vma=False)
```

```python
import math

import jax
import jax.numpy as jnp
import numpy as np
from jax import lax
from jax.experimental import pallas as pl
from jax.experimental.pallas import tpu as pltpu
from jax.sharding import Mesh
from jax.sharding import PartitionSpec as P

tv_weight = 0.15
smoothing = 0.6
f32 = jnp.float32
bf16 = jnp.bfloat16

LANE = 128
HALF = 64
WIDE = 384


def dft(length, direction):
    counter = np.arange(length)
    angle = (counter[:, None] * counter[None, :] % length).astype(np.float32) * np.float32(2.0 * math.pi / length)
    factor = np.float32(1.0 / math.sqrt(length))
    return np.cos(angle) * factor, np.float32(direction) * np.sin(angle) * factor


def column_table(length, direction):
    real, imag = dft(length, direction)
    whole = np.concatenate(
        [np.concatenate([real, imag], axis=1), np.concatenate([-imag, real], axis=1)], axis=0
    )
    order = np.concatenate(
        [
            np.arange(LANE),
            length + np.arange(LANE),
            np.arange(LANE, length),
            length + np.arange(LANE, length),
        ]
    )
    packed = whole[order][:, order]
    tail = np.concatenate([-packed[:, WIDE - HALF :], packed[:, WIDE - LANE : WIDE - HALF]], axis=1)
    return jnp.asarray(np.concatenate([packed, tail], axis=1), dtype=bf16)


def depth_table(length, direction):
    real, imag = dft(length, direction)
    return jnp.asarray(
        np.concatenate(
            [np.concatenate([real, -imag], axis=1), np.concatenate([imag, real], axis=1)], axis=0
        ),
        dtype=bf16,
    )


def dot(a, b):
    return jnp.dot(a, b, preferred_element_type=f32)


def lanes(*pieces):
    return jnp.concatenate(pieces, axis=1)


def stack(*pieces):
    return jnp.concatenate(pieces, axis=0)


def left_half(shape):
    return lax.broadcasted_iota(jnp.int32, shape, 1) < HALF


def swapped(d):
    return pltpu.roll(d, HALF, 1)


def times_i(d):
    other = swapped(d)
    return jnp.where(left_half(d.shape), -other, other)


def doubled(d):
    other = swapped(d)
    left = left_half(d.shape)
    return jnp.where(left, d, other), jnp.where(left, other, d)


def mask_lanes(mask):
    mask = mask.astype(f32)
    return mask[:, :LANE], lanes(mask[:, LANE:], mask[:, LANE:])


def call(kernel, flops, **kwargs):
    return pl.pallas_call(
        kernel,
        cost_estimate=pl.CostEstimate(flops=flops, transcendentals=0, bytes_accessed=2**20),
        compiler_params=pltpu.CompilerParams(vmem_limit_bytes=32 * 2**20),
        **kwargs,
    )


VMEM = pl.BlockSpec(memory_space=pltpu.VMEM)


def distant(value):
    return pltpu.with_memory_space_constraint(value, pltpu.HBM)


def depart(data, sampling, coils, depth_inv, nhi, group):
    encodings, rows, slices, _ = data.shape[1:]
    images = encodings * rows

    slabs = slices // 2

    def kernel(data_ref, mask_ref, coil_ref, table, out):
        share_index = lax.axis_index("phase") * lax.axis_size("enc") + lax.axis_index("enc")
        for e in range(encodings):
            weight = -mask_ref[e].astype(f32)
            for r in range(rows):
                both = stack(*((data_ref[c, e, r].astype(f32) * weight).astype(bf16) for c in range(2)))
                both = dot(table[...], both)
                real, imag = both[:slices], both[slices:]
                at = (e * rows + r) * WIDE
                for j, x in enumerate((real[:, :LANE], imag[:, :LANE], lanes(real[:, LANE:], imag[:, LANE:]))):
                    x = x.astype(bf16).reshape(slabs, 2, LANE)
                    out[:, :, at + j * LANE : at + (j + 1) * LANE] = x
        first = share_index * group
        for k in range(group):
            real, imag = (coil_ref[c, first + k].astype(f32) for c in range(2))
            tail = jnp.concatenate([real[:, :, LANE:], imag[:, :, LANE:]], axis=2)
            at = (images + k) * WIDE
            for j, x in enumerate((real[:, :, :LANE], imag[:, :, :LANE], tail)):
                x = x.astype(bf16)
                for h in range(nhi):
                    out[4 * h : 4 * h + 4, :, at + j * LANE : at + (j + 1) * LANE] = x

    return call(
        kernel,
        10**8,
        in_specs=[VMEM, VMEM, VMEM, VMEM],
        out_specs=VMEM,
        out_shape=jax.ShapeDtypeStruct((slabs, 2, (images + group) * WIDE), bf16),
    )(*(distant(a) for a in (data, sampling, coils, depth_inv)))


def slab_gradient(packed, coil_rows, column_inv, encodings, nhi):
    rows, _, slices, _ = coil_rows.shape

    def kernel(in_ref, coil_ref, table, out, send):
        images = [in_ref[:, i * WIDE : (i + 1) * WIDE] for i in range(encodings * rows)]
        fine = dot(stack(*images), table[...])
        coil = []
        for r in range(rows):
            real, imag = coil_ref[r, 0].astype(f32), coil_ref[r, 1].astype(f32)
            coil.append(
                (
                    real[:, :LANE],
                    imag[:, :LANE],
                    lanes(real[:, LANE:], real[:, LANE:]),
                    lanes(imag[:, LANE:], imag[:, LANE:]),
                )
            )
        even = lax.rem(lax.broadcasted_iota(jnp.int32, (8, WIDE), 0) // 2, 2) == 0
        for e in range(encodings):
            total = jnp.zeros((8, WIDE), f32)
            for r in range(rows):
                at = (e * rows + r) * slices
                a, b, d, t = (fine[at : at + slices, j * LANE : (j + 1) * LANE] for j in range(4))
                ca, cb, dr, di = coil[r]
                value = lanes(ca * a + cb * b, ca * b - cb * a, dr * d - di * t)
                value = jnp.sum(value.reshape(slices // 8, 8, WIDE), axis=0)
                turned = (-2 * r) % 8
                one = value if turned == 0 else pltpu.roll(value, turned, 0)
                two = pltpu.roll(value, (turned + 4) % 8, 0) if (turned + 4) % 8 else value
                total = total + jnp.where(even, one, two)
            for x in range(4):
                mine = pltpu.roll(total, 8 - 2 * x, 0) if x else total
                out[x, :, e * WIDE : (e + 1) * WIDE] = mine
                for h in range(nhi):
                    send[4 * h + x, :, e * WIDE : (e + 1) * WIDE] = mine[:2].astype(bf16)

    return call(
        kernel,
        10**8,
        in_specs=[VMEM, VMEM, VMEM],
        out_specs=[VMEM, VMEM],
        out_shape=[
            jax.ShapeDtypeStruct((4, 8, encodings * WIDE), f32),
            jax.ShapeDtypeStruct((slices // 2, 2, encodings * WIDE), bf16),
        ],
    )(packed, coil_rows, column_inv)


def step_length(norm_ref):
    gg, ee = (jnp.sum(norm_ref[:, i : i + 1, :], axis=0) for i in range(2))
    return gg / (ee + 4.0 * tv_weight / smoothing * gg + 1e-06)


def whole(array):
    return pl.BlockSpec(array.shape, lambda g, _n=len(array.shape): (0,) * _n)


def coil_lanes(ref, step, k):
    a, b, d = (ref[step, :, k * WIDE + j * LANE : k * WIDE + (j + 1) * LANE].astype(f32) for j in range(3))
    return (a, b, *doubled(d))


def forward_step(image, extra, sampling, own, other, tables, members, second):
    column_fwd, _, depth_fwd, depth_inv = tables
    slices, width = image.shape
    encodings = width // WIDE
    steps = own.shape[0]
    group = own.shape[2] // WIDE
    nlo = 4

    def kernel(*refs):
        refs = list(refs)
        if second:
            norms_ref, image_ref, before_ref, after_ref, normal_ref, *firsts = (refs.pop(0) for _ in range(8))
        else:
            image_ref = refs.pop(0)
        mask_ref, own_ref, other_ref, wf, zf, zi = (refs.pop(0) for _ in range(6))
        sends = [refs.pop(0) for _ in range(3)]
        norm_ref, out_ref = refs.pop(0), refs.pop(0)
        value, ahead_ref, mask_a, mask_d, product, squares, *spectra = refs
        spectrum = spectra[0] if second else out_ref
        only = lambda condition: (lambda f: f()) if second else pl.when(condition)
        hi, lo, core = (lax.axis_index(name) for name in ("hi", "lo", "enc"))

        def column(ref, e, j):
            at = e * WIDE + j * LANE
            return ref[:, at : at + LANE].astype(f32)

        @only(pl.program_id(0) == 0 if not second else True)
        def _():
            total = jnp.zeros((slices, LANE), f32)
            for e in range(encodings):
                now = [column(image_ref, e, j) for j in range(3)]
                if second:
                    alpha = step_length(norms_ref)
                    new = [-alpha * v for v in now]
                    slopes = []
                    for d in (
                        [new[j] + alpha * column(before_ref, e, j) for j in range(3)],
                        [-alpha * column(after_ref, e, j) - new[j] for j in range(3)],
                    ):
                        close = jnp.sqrt(d[0] * d[0] + d[1] * d[1] + smoothing * smoothing)
                        square = d[2] * d[2]
                        far = jnp.sqrt(square + swapped(square) + smoothing * smoothing)
                        slopes.append([d[0] / close, d[1] / close, d[2] / far])
                    now = [
                        now[j] - alpha * column(normal_ref, e, j) + tv_weight * (slopes[0][j] - slopes[1][j])
                        for j in range(3)
                    ]
                    for j in range(3):
                        at = e * WIDE + j * LANE
                        ahead_ref[:, at : at + LANE] = now[j]
                for j in range(3):
                    total = total + now[j] * now[j]
                    now[j] = now[j].astype(bf16).astype(f32)
                    value[:, e * 512 + j * LANE : e * 512 + (j + 1) * LANE] = now[j]
                value[:, e * 512 + 3 * LANE : (e + 1) * 512] = times_i(now[2])
                a, d = mask_lanes(mask_ref[e])
                mask_a[:, e * LANE : (e + 1) * LANE] = a
                mask_d[:, e * LANE : (e + 1) * LANE] = d
            norm_ref[:, 0:1, :] = jnp.full((members, 1, LANE), jnp.sum(total), f32)
            squares[...] = jnp.zeros(squares.shape, f32)

        def one_step(step, carry):
            at_step = step if second else 0
            for half, coil_ref in ((0, own_ref), (1, other_ref)):
                for k in range(group):
                    ca, cb, dr, di = coil_lanes(coil_ref, at_step, k)
                    for e in range(encodings):
                        va, vb, vd, vt = (value[:, e * 512 + j * LANE : e * 512 + (j + 1) * LANE] for j in range(4))
                        at = ((half * group + k) * encodings + e) * slices
                        product[at : at + slices, :LANE] = (ca * va - cb * vb).astype(bf16)
                        product[at : at + slices, LANE : 2 * LANE] = (ca * vb + cb * va).astype(bf16)
                        product[at : at + slices, 2 * LANE :] = (dr * vd + di * vt).astype(bf16)
            weight_a, weight_d = mask_a[...], mask_d[...]
            total = jnp.zeros(weight_a.shape, f32)
            rows = group * encodings * slices
            for half in range(2):
                u = dot(product[half * rows : (half + 1) * rows, :], wf[...]).astype(bf16)
                for k in range(group):

                    def pair(j):
                        return lanes(
                            *(
                                u[(k * encodings + e) * slices : (k * encodings + e + 1) * slices, j * LANE : (j + 1) * LANE]
                                for e in range(encodings)
                            )
                        )

                    close = dot(zf[...], stack(pair(0), pair(1)))
                    far = dot(zi[...], stack(pair(2), pair(3)))
                    sa, sb = close[:slices] * weight_a, close[slices:] * weight_a
                    sd, st = far[:slices] * weight_d, far[slices:] * weight_d
                    total = total + (sa * sa + sb * sb + sd * sd)
                    for j, x in enumerate((sa, sb, sd, st)):
                        spectrum[half * group + k, :, j * 2 * LANE : (j + 1) * 2 * LANE] = x.astype(bf16)
            squares[...] += total
            for half in range(2):
                owner = 2 * step + (core if half == 0 else 1 - core)

                @pl.when(owner == hi)
                def _():
                    for j, send_ref in enumerate(sends):
                        dest = lax.bitwise_xor(lo, j)
                        coil = (3 * dest + lax.rem(lo + dest, nlo)) // nlo
                        send_ref[:slices] = spectrum[half * group + coil, :, :width]

            return carry

        if second:
            lax.fori_loop(0, steps, one_step, 0)
        else:
            one_step(pl.program_id(0), 0)
        if second:
            piece = ahead_ref[pl.ds(pl.multiple_of(8 * hi, 8), 8), :]
            turned = [pltpu.roll(piece, 8 - 2 * dest, 0) if dest else piece for dest in range(nlo)]
            for j in range(nlo):
                dest = lax.bitwise_xor(lo, j)
                part = turned[0]
                for k in range(1, nlo):
                    part = jnp.where(dest == k, turned[k], part)
                part = stack(part, part).astype(bf16)
                if j < 3:
                    sends[j][slices : slices + 16] = part
                    sends[j][slices + 16 :] = firsts[j][...]
                else:
                    out_ref[...] = part

        @only(pl.program_id(0) == steps - 1 if not second else True)
        def _():
            norm_ref[:, 1:2, :] = jnp.full((members, 1, LANE), jnp.sum(squares[...]), f32)

    arrays = [*extra[:1], image, *extra[1:], sampling, own, other, column_fwd, depth_fwd, depth_inv]
    wide = encodings * 512
    norms = jax.ShapeDtypeStruct((members, 2, LANE), f32)
    scratch = [
        pltpu.VMEM((slices, wide), f32),
        pltpu.VMEM((slices, width), f32),
        pltpu.VMEM((slices, encodings * LANE), f32),
        pltpu.VMEM((slices, encodings * LANE), f32),
        pltpu.VMEM((2 * group * encodings * slices, WIDE), bf16),
        pltpu.VMEM((slices, encodings * LANE), f32),
    ]
    if second:
        outs = [jax.ShapeDtypeStruct((2 * slices + 16, width), bf16)] * 3
        return call(
            kernel,
            2 * 10**9,
            in_specs=[VMEM] * len(arrays),
            out_specs=[VMEM] * 5,
            out_shape=[*outs, norms, jax.ShapeDtypeStruct((16, width), bf16)],
            scratch_shapes=[*scratch, pltpu.VMEM((2 * group, slices, wide), bf16)],
        )(*(distant(a) if i > 3 and i < 8 else a for i, a in enumerate(arrays)))
    outs = [pltpu.HBM((slices, width), bf16)] * 3 + [norms]
    coil_spec = pl.BlockSpec((1,) + own.shape[1:], lambda g: (g, 0, 0))
    spectrum_spec = pl.BlockSpec((2 * group, slices, wide), lambda g: (g, 0, 0))
    return call(
        kernel,
        2 * 10**9,
        grid=(steps,),
        in_specs=[whole(image), whole(sampling), coil_spec, coil_spec, *(whole(a) for a in arrays[4:])],
        out_specs=[*(whole(o) for o in outs), spectrum_spec],
        out_shape=[*outs, pltpu.HBM((steps * 2 * group, slices, wide), bf16)],
        scratch_shapes=scratch,
    )(*arrays)


def adjoint_step(spectrum, own, other, tables, width):
    _, column_inv, depth_fwd, depth_inv = tables
    _, slices, wide = spectrum.shape
    encodings = wide // 512
    steps = own.shape[0]
    group = own.shape[2] // WIDE

    def kernel(spectrum_ref, own_ref, other_ref, wi, zf, zi, out_ref, product):
        @pl.when(pl.program_id(0) == 0)
        def _():
            out_ref[...] = jnp.zeros(out_ref.shape, f32)

        def one_step():
            for half in range(2):
                for k in range(group):
                    sa, sb, sd, st = (
                        spectrum_ref[half * group + k, :, j * 2 * LANE : (j + 1) * 2 * LANE]
                        for j in range(4)
                    )
                    close = dot(zi[...], stack(sa, sb)).astype(bf16)
                    far = dot(zf[:slices, :], stack(sd, st)).astype(bf16)
                    for e in range(encodings):
                        at = ((half * group + k) * encodings + e) * slices
                        for j, x in enumerate((close[:slices], close[slices:], far)):
                            product[at : at + slices, j * LANE : (j + 1) * LANE] = x[:, e * LANE : (e + 1) * LANE]
            rows = group * encodings * slices
            sums = [[0.0, 0.0, 0.0] for _ in range(encodings)]
            for half, coil_ref in ((0, own_ref), (1, other_ref)):
                q = dot(product[half * rows : (half + 1) * rows, :], wi[...])
                for k in range(group):
                    ca, cb, dr, di = coil_lanes(coil_ref, 0, k)
                    for e in range(encodings):
                        at = (k * encodings + e) * slices
                        qa, qb, qd, qt = (q[at : at + slices, j * LANE : (j + 1) * LANE] for j in range(4))
                        sums[e][0] += ca * qa + cb * qb
                        sums[e][1] += ca * qb - cb * qa
                        sums[e][2] += dr * qd - di * qt
            for e in range(encodings):
                for j in range(3):
                    at = e * WIDE + j * LANE
                    out_ref[:, at : at + LANE] += sums[e][j]

        one_step()

    arrays = [spectrum, own, other, column_inv, depth_fwd, depth_inv]
    coil_spec = pl.BlockSpec((1,) + own.shape[1:], lambda g: (g, 0, 0))
    spectrum_spec = pl.BlockSpec((2 * group, slices, wide), lambda g: (g, 0, 0))
    out = pltpu.HBM((slices, width), f32)
    return call(
        kernel,
        2 * 10**9,
        grid=(steps,),
        in_specs=[spectrum_spec, coil_spec, coil_spec, *(whole(a) for a in arrays[3:])],
        out_specs=whole(out),
        out_shape=out,
        scratch_shapes=[pltpu.VMEM((2 * group * encodings * slices, WIDE), bf16)],
    )(distant(spectrum), *arrays[1:])


def finish(norms_one, norms_two, data, sampling, slab_one, rows, last, readout):
    encodings, nrows, slices, lines = data.shape[1:]

    def kernel(norm_one, norm_two, data_ref, mask_ref, slab, keep, one, two, last_ref, out, image):
        lo = lax.axis_index("lo")
        alphas = step_length(norm_one), step_length(norm_two)
        for j, rows_ref in enumerate((keep, one, two)):
            r = jnp.where(lax.rem(lo, 2) == 0, j, nrows - 1 - j)
            for e in range(encodings):
                weight = mask_ref[e].astype(f32)
                real, imag = (-(data_ref[c, e, r].astype(f32) * weight) for c in range(2))
                a, b, d = (
                    alphas[0] * rows_ref[slices + 16 :, (2 * k + e) * LANE : (2 * k + e + 1) * LANE].astype(f32)
                    + alphas[1] * rows_ref[:slices, (2 * k + e) * LANE : (2 * k + e + 1) * LANE].astype(f32)
                    for k in range(3)
                )
                out[0, e, r, :, :LANE] = real[:, :LANE] - a
                out[1, e, r, :, :LANE] = imag[:, :LANE] - b
                out[0, e, r, :, LANE:] = real[:, LANE:] - d[:, :HALF]
                out[1, e, r, :, LANE:] = imag[:, LANE:] - swapped(d)[:, :HALF]
        for j in range(readout):
            x = lax.bitwise_xor(lo, j)
            for e in range(encodings):
                for k in range(3):
                    at = e * WIDE + k * LANE
                    if j < 3:
                        step = (keep, one, two)[j][slices : slices + 16, at : at + LANE]
                    else:
                        step = last_ref[:, at : at + LANE]
                    value = -alphas[0] * slab[x, :, at : at + LANE] - alphas[1] * step.astype(f32)[:8]
                    if k < 2:
                        image[k, e, x, :, :LANE] = value[:2]
                    else:
                        image[0, e, x, :, LANE:] = value[:2, :HALF]
                        image[1, e, x, :, LANE:] = swapped(value)[:2, :HALF]

    return call(
        kernel,
        10**7,
        in_specs=[VMEM] * 9,
        out_specs=[VMEM, VMEM],
        out_shape=[
            jax.ShapeDtypeStruct(data.shape, f32),
            jax.ShapeDtypeStruct((2, encodings, readout, 2, lines), f32),
        ],
    )(norms_one, norms_two, data, sampling, slab_one, *rows, last)


def reconstruct(kspace_data, coil_maps, sampling):
    encodings = kspace_data.shape[2]
    rows = kspace_data.shape[3]
    slices = kspace_data.shape[4]
    coils, readout, zdepth, lines = coil_maps.shape[1:]
    nhi, nlo = lax.axis_size("hi"), lax.axis_size("lo")
    nphase, ncore = lax.axis_size("phase"), lax.axis_size("enc")
    slabs = nhi * nlo
    group = coils // (nphase * ncore)
    assert (nlo, readout, rows, zdepth, lines, slices) == (4, 4, 3, 2, LANE + HALF, 2 * slabs)
    assert group * nhi == coils and nphase * ncore == nhi and ncore == 2
    column_fwd, column_inv = column_table(lines, -1.0), column_table(lines, 1.0)
    depth_fwd, depth_inv = depth_table(slices, -1.0), depth_table(slices, 1.0)
    tables = (column_fwd, column_inv, depth_fwd, depth_inv)
    sampling = sampling[0]
    data = kspace_data[:, 0]

    def round_ring(value):
        value = value.reshape(slabs, zdepth, -1)
        return lax.all_to_all(value, ("hi", "lo"), 0, 0, tiled=True).reshape(slices, -1)

    packed = depart(data, sampling, coil_maps, depth_inv, nhi, group)
    packed = round_ring(packed)
    coil_rows = coil_maps.reshape(2, slabs, rows, zdepth, lines).transpose(2, 0, 1, 3, 4)
    coil_rows = coil_rows.reshape(rows, 2, slices, lines)
    slab_one, spread = slab_gradient(packed, coil_rows, column_inv, encodings, nhi)
    one = round_ring(spread)
    own = lax.all_gather(packed[:, encodings * rows * WIDE :], "phase")
    other = lax.ppermute(own, "enc", [(i, (i + 1) % ncore) for i in range(ncore)])

    up = [(i, (i + 1) % nphase) for i in range(nphase)]
    before = lax.ppermute(one, "phase", up)
    after = lax.ppermute(one, "phase", [(j, i) for i, j in up])

    def total(norms):
        return lax.all_to_all(norms, ("lo", "phase", "enc"), 0, 0, tiled=True)

    members = nlo * nphase * ncore

    def swap(value, j):
        return lax.ppermute(value, "lo", [(i, i ^ j) for i in range(nlo)])

    *rows_one, norms, spectrum = forward_step(one, (), sampling, own, other, tables, members, False)
    norms_one = total(norms)
    normal = adjoint_step(spectrum, own, other, tables, one.shape[1])
    extra = (norms_one, before, after, normal, *rows_one)
    *rows_two, norms, last = forward_step(one, extra, sampling, own, other, tables, members, True)
    near = swap(rows_two[1], 1)
    far = swap(rows_two[2], 2)
    norms_two = total(norms)
    last = swap(last, 3)
    got = [rows_two[0], near, far]
    residual, image = finish(norms_one, norms_two, data, sampling, slab_one, got, last, readout)
    return (image[:, None], residual[:, None])


def solution(mesh):
    names = dict(mesh.shape)
    nlo = 4
    grid = Mesh(
        mesh.devices.reshape(names["pat"], names["slab"] // nlo, nlo, names["phase"], names["enc"]),
        ("pat", "hi", "lo", "phase", "enc"),
    )
    slab = ("hi", "lo")
    in_specs = (
        P("pat", "phase", "enc", slab, None, None),
        P("pat", None, None, slab, None),
        P("phase", "enc", "pat", None),
    )
    out_specs = (
        P("pat", "phase", "enc", None, slab, None),
        P("pat", "phase", "enc", slab, None, None),
    )
    return jax.shard_map(reconstruct, mesh=grid, in_specs=in_specs, out_specs=out_specs, check_vma=False)
```

```python
import math

import jax
import jax.numpy as jnp
import numpy as np
from jax import lax
from jax.experimental import pallas as pl
from jax.experimental.pallas import tpu as pltpu
from jax.sharding import Mesh
from jax.sharding import PartitionSpec as P

tv_weight = 0.15
smoothing = 0.6
f32 = jnp.float32
bf16 = jnp.bfloat16

LANE = 128
HALF = 64
WIDE = 384


def dft(length, direction):
    counter = np.arange(length)
    angle = (counter[:, None] * counter[None, :] % length).astype(np.float32) * np.float32(2.0 * math.pi / length)
    factor = np.float32(1.0 / math.sqrt(length))
    return np.cos(angle) * factor, np.float32(direction) * np.sin(angle) * factor


def column_table(length, direction):
    real, imag = dft(length, direction)
    whole = np.concatenate(
        [np.concatenate([real, imag], axis=1), np.concatenate([-imag, real], axis=1)], axis=0
    )
    order = np.concatenate(
        [
            np.arange(LANE),
            length + np.arange(LANE),
            np.arange(LANE, length),
            length + np.arange(LANE, length),
        ]
    )
    packed = whole[order][:, order]
    tail = np.concatenate([-packed[:, WIDE - HALF :], packed[:, WIDE - LANE : WIDE - HALF]], axis=1)
    return jnp.asarray(np.concatenate([packed, tail], axis=1), dtype=bf16)


def depth_table(length, direction):
    real, imag = dft(length, direction)
    return jnp.asarray(
        np.concatenate(
            [np.concatenate([real, -imag], axis=1), np.concatenate([imag, real], axis=1)], axis=0
        ),
        dtype=bf16,
    )


def dot(a, b):
    return jnp.dot(a, b, preferred_element_type=f32)


def lanes(*pieces):
    return jnp.concatenate(pieces, axis=1)


def stack(*pieces):
    return jnp.concatenate(pieces, axis=0)


def left_half(shape):
    return lax.broadcasted_iota(jnp.int32, shape, 1) < HALF


def swapped(d):
    return pltpu.roll(d, HALF, 1)


def times_i(d):
    other = swapped(d)
    return jnp.where(left_half(d.shape), -other, other)


def doubled(d):
    other = swapped(d)
    left = left_half(d.shape)
    return jnp.where(left, d, other), jnp.where(left, other, d)


def mask_lanes(mask):
    mask = mask.astype(f32)
    return mask[:, :LANE], lanes(mask[:, LANE:], mask[:, LANE:])


def call(kernel, flops, **kwargs):
    return pl.pallas_call(
        kernel,
        cost_estimate=pl.CostEstimate(flops=flops, transcendentals=0, bytes_accessed=2**20),
        compiler_params=pltpu.CompilerParams(vmem_limit_bytes=32 * 2**20),
        **kwargs,
    )


VMEM = pl.BlockSpec(memory_space=pltpu.VMEM)


def distant(value):
    return pltpu.with_memory_space_constraint(value, pltpu.HBM)


def depart(data, sampling, coils, depth_inv, nhi, group):
    encodings, rows, slices, _ = data.shape[1:]
    images = encodings * rows

    slabs = slices // 2

    def kernel(data_ref, mask_ref, coil_ref, table, out):
        share_index = lax.axis_index("phase") * lax.axis_size("enc") + lax.axis_index("enc")
        for e in range(encodings):
            weight = -mask_ref[e].astype(f32)
            for r in range(rows):
                both = stack(*((data_ref[c, e, r].astype(f32) * weight).astype(bf16) for c in range(2)))
                both = dot(table[...], both)
                real, imag = both[:slices], both[slices:]
                at = (e * rows + r) * WIDE
                for j, x in enumerate((real[:, :LANE], imag[:, :LANE], lanes(real[:, LANE:], imag[:, LANE:]))):
                    x = x.astype(bf16).reshape(slabs, 2, LANE)
                    out[:, :, at + j * LANE : at + (j + 1) * LANE] = x
        first = share_index * group
        for k in range(group):
            real, imag = (coil_ref[c, first + k].astype(f32) for c in range(2))
            tail = jnp.concatenate([real[:, :, LANE:], imag[:, :, LANE:]], axis=2)
            at = (images + k) * WIDE
            for j, x in enumerate((real[:, :, :LANE], imag[:, :, :LANE], tail)):
                x = x.astype(bf16)
                for h in range(nhi):
                    out[4 * h : 4 * h + 4, :, at + j * LANE : at + (j + 1) * LANE] = x

    return call(
        kernel,
        10**8,
        in_specs=[VMEM, VMEM, VMEM, VMEM],
        out_specs=VMEM,
        out_shape=jax.ShapeDtypeStruct((slabs, 2, (images + group) * WIDE), bf16),
    )(*(distant(a) for a in (data, sampling, coils, depth_inv)))


def slab_gradient(packed, coil_rows, column_inv, encodings, nhi):
    rows, _, slices, _ = coil_rows.shape

    def kernel(in_ref, coil_ref, table, out, send):
        images = [in_ref[:, i * WIDE : (i + 1) * WIDE] for i in range(encodings * rows)]
        fine = dot(stack(*images), table[...])
        coil = []
        for r in range(rows):
            real, imag = coil_ref[r, 0].astype(f32), coil_ref[r, 1].astype(f32)
            coil.append(
                (
                    real[:, :LANE],
                    imag[:, :LANE],
                    lanes(real[:, LANE:], real[:, LANE:]),
                    lanes(imag[:, LANE:], imag[:, LANE:]),
                )
            )
        even = lax.rem(lax.broadcasted_iota(jnp.int32, (8, WIDE), 0) // 2, 2) == 0
        for e in range(encodings):
            total = jnp.zeros((8, WIDE), f32)
            for r in range(rows):
                at = (e * rows + r) * slices
                a, b, d, t = (fine[at : at + slices, j * LANE : (j + 1) * LANE] for j in range(4))
                ca, cb, dr, di = coil[r]
                value = lanes(ca * a + cb * b, ca * b - cb * a, dr * d - di * t)
                value = jnp.sum(value.reshape(slices // 8, 8, WIDE), axis=0)
                turned = (-2 * r) % 8
                one = value if turned == 0 else pltpu.roll(value, turned, 0)
                two = pltpu.roll(value, (turned + 4) % 8, 0) if (turned + 4) % 8 else value
                total = total + jnp.where(even, one, two)
            for x in range(4):
                mine = pltpu.roll(total, 8 - 2 * x, 0) if x else total
                out[x, :, e * WIDE : (e + 1) * WIDE] = mine
                for h in range(nhi):
                    send[4 * h + x, :, e * WIDE : (e + 1) * WIDE] = mine[:2].astype(bf16)

    return call(
        kernel,
        10**8,
        in_specs=[VMEM, VMEM, VMEM],
        out_specs=[VMEM, VMEM],
        out_shape=[
            jax.ShapeDtypeStruct((4, 8, encodings * WIDE), f32),
            jax.ShapeDtypeStruct((slices // 2, 2, encodings * WIDE), bf16),
        ],
    )(packed, coil_rows, column_inv)


def step_length(norm_ref):
    gg, ee = (jnp.sum(norm_ref[:, i : i + 1, :], axis=0) for i in range(2))
    return gg / (ee + 4.0 * tv_weight / smoothing * gg + 1e-06)


def whole(array):
    return pl.BlockSpec(array.shape, lambda g, _n=len(array.shape): (0,) * _n)


def coil_lanes(ref, step, k):
    a, b, d = (ref[step, :, k * WIDE + j * LANE : k * WIDE + (j + 1) * LANE].astype(f32) for j in range(3))
    return (a, b, *doubled(d))


def forward_step(image, extra, sampling, own, other, tables, members, second):
    column_fwd, _, depth_fwd, depth_inv = tables
    slices, width = image.shape
    encodings = width // WIDE
    steps = own.shape[0]
    group = own.shape[2] // WIDE
    nlo = 4

    def kernel(*refs):
        refs = list(refs)
        if second:
            norms_ref, image_ref, before_ref, after_ref, normal_ref, *firsts = (refs.pop(0) for _ in range(8))
        else:
            image_ref = refs.pop(0)
        mask_ref, own_ref, other_ref, wf, zf, zi = (refs.pop(0) for _ in range(6))
        sends = [refs.pop(0) for _ in range(3)]
        norm_ref, out_ref = refs.pop(0), refs.pop(0)
        value, ahead_ref, mask_a, mask_d, product, squares, *spectra = refs
        spectrum = spectra[0] if second else out_ref
        copies = []
        if second:
            for j in range(3):
                copies.append(
                    pltpu.make_async_copy(firsts[j], sends[j].at[pl.ds(slices + 16, slices)], spectra[1].at[j])
                )
            copies.append(pltpu.make_async_copy(normal_ref, spectra[2], spectra[1].at[3]))
            for copy in reversed(copies):
                copy.start()
        only = lambda condition: (lambda f: f()) if second else pl.when(condition)
        hi, lo, core = (lax.axis_index(name) for name in ("hi", "lo", "enc"))

        def column(ref, e, j):
            at = e * WIDE + j * LANE
            return ref[:, at : at + LANE].astype(f32)

        @only(pl.program_id(0) == 0 if not second else True)
        def _():
            total = jnp.zeros((slices, LANE), f32)
            for e in range(encodings):
                now = [column(image_ref, e, j) for j in range(3)]
                if second:
                    alpha = step_length(norms_ref)
                    new = [-alpha * v for v in now]
                    slopes = []
                    for d in (
                        [new[j] + alpha * column(before_ref, e, j) for j in range(3)],
                        [-alpha * column(after_ref, e, j) - new[j] for j in range(3)],
                    ):
                        close = jnp.sqrt(d[0] * d[0] + d[1] * d[1] + smoothing * smoothing)
                        square = d[2] * d[2]
                        far = jnp.sqrt(square + swapped(square) + smoothing * smoothing)
                        slopes.append([d[0] / close, d[1] / close, d[2] / far])
                    now = [now[j] + tv_weight * (slopes[0][j] - slopes[1][j]) for j in range(3)]
                    for j in range(3):
                        at = e * WIDE + j * LANE
                        ahead_ref[:, at : at + LANE] = now[j]
            if second:
                copies[3].wait()
            for e in range(encodings):
                now = [column(image_ref, e, j) for j in range(3)]
                if second:
                    now = [column(ahead_ref, e, j) - alpha * column(spectra[2], e, j) for j in range(3)]
                    for j in range(3):
                        at = e * WIDE + j * LANE
                        ahead_ref[:, at : at + LANE] = now[j]
                for j in range(3):
                    total = total + now[j] * now[j]
                    now[j] = now[j].astype(bf16).astype(f32)
                    value[:, e * 512 + j * LANE : e * 512 + (j + 1) * LANE] = now[j]
                value[:, e * 512 + 3 * LANE : (e + 1) * 512] = times_i(now[2])
                a, d = mask_lanes(mask_ref[e])
                mask_a[:, e * LANE : (e + 1) * LANE] = a
                mask_d[:, e * LANE : (e + 1) * LANE] = d
            norm_ref[:, 0:1, :] = jnp.full((members, 1, LANE), jnp.sum(total), f32)
            squares[...] = jnp.zeros(squares.shape, f32)

        def one_step(step, carry):
            at_step = step if second else 0
            for half, coil_ref in ((0, own_ref), (1, other_ref)):
                for k in range(group):
                    ca, cb, dr, di = coil_lanes(coil_ref, at_step, k)
                    for e in range(encodings):
                        va, vb, vd, vt = (value[:, e * 512 + j * LANE : e * 512 + (j + 1) * LANE] for j in range(4))
                        at = ((half * group + k) * encodings + e) * slices
                        product[at : at + slices, :LANE] = (ca * va - cb * vb).astype(bf16)
                        product[at : at + slices, LANE : 2 * LANE] = (ca * vb + cb * va).astype(bf16)
                        product[at : at + slices, 2 * LANE :] = (dr * vd + di * vt).astype(bf16)
            weight_a, weight_d = mask_a[...], mask_d[...]
            total = jnp.zeros(weight_a.shape, f32)
            u = dot(product[...], wf[...]).astype(bf16)
            for k in range(2 * group):

                def pair(j):
                    return lanes(
                        *(
                            u[(k * encodings + e) * slices : (k * encodings + e + 1) * slices, j * LANE : (j + 1) * LANE]
                            for e in range(encodings)
                        )
                    )

                close = dot(zf[...], stack(pair(0), pair(1)))
                sd = dot(zi[:slices, :], stack(pair(2), pair(3))) * weight_d
                sa, sb = close[:slices] * weight_a, close[slices:] * weight_a
                total = total + (sa * sa + sb * sb + sd * sd)
                parts = [sa, sb, sd]
                if not second:
                    parts.append(lanes(*(times_i(sd[:, e * LANE : (e + 1) * LANE]) for e in range(encodings))))
                for j, x in enumerate(parts):
                    spectrum[k, :, j * 2 * LANE : (j + 1) * 2 * LANE] = x.astype(bf16)
            squares[...] += total
            for half in range(2):
                owner = 2 * step + (core if half == 0 else 1 - core)

                @pl.when(owner == hi)
                def _():
                    for j, send_ref in enumerate(sends):
                        dest = lax.bitwise_xor(lo, j)
                        coil = (3 * dest + lax.rem(lo + dest, nlo)) // nlo
                        send_ref[:slices] = spectrum[half * group + coil, :, :width]

            return carry

        if second:
            lax.fori_loop(0, steps, one_step, 0)
        else:
            one_step(pl.program_id(0), 0)
        if second:
            piece = ahead_ref[pl.ds(pl.multiple_of(8 * hi, 8), 8), :]
            turned = [pltpu.roll(piece, 8 - 2 * dest, 0) if dest else piece for dest in range(nlo)]
            for j in range(nlo):
                dest = lax.bitwise_xor(lo, j)
                part = turned[0]
                for k in range(1, nlo):
                    part = jnp.where(dest == k, turned[k], part)
                part = stack(part, part).astype(bf16)
                if j < 3:
                    sends[j][slices : slices + 16] = part
                    copies[j].wait()
                else:
                    out_ref[...] = part

        @only(pl.program_id(0) == steps - 1 if not second else True)
        def _():
            norm_ref[:, 1:2, :] = jnp.full((members, 1, LANE), jnp.sum(squares[...]), f32)

    arrays = [*extra[:1], image, *extra[1:], sampling, own, other, column_fwd, depth_fwd, depth_inv]
    wide = encodings * 512
    norms = jax.ShapeDtypeStruct((members, 2, LANE), f32)
    scratch = [
        pltpu.VMEM((slices, wide), f32),
        pltpu.VMEM((slices, width), f32),
        pltpu.VMEM((slices, encodings * LANE), f32),
        pltpu.VMEM((slices, encodings * LANE), f32),
        pltpu.VMEM((2 * group * encodings * slices, WIDE), bf16),
        pltpu.VMEM((slices, encodings * LANE), f32),
    ]
    if second:
        outs = [jax.ShapeDtypeStruct((2 * slices + 16, width), bf16)] * 3
        return call(
            kernel,
            2 * 10**9,
            in_specs=[VMEM] * 4 + [pl.BlockSpec(memory_space=pl.ANY)] * 4 + [VMEM] * (len(arrays) - 8),
            out_specs=[VMEM] * 5,
            out_shape=[*outs, norms, jax.ShapeDtypeStruct((16, width), bf16)],
            scratch_shapes=[*scratch, pltpu.VMEM((2 * group, slices, width), bf16), pltpu.SemaphoreType.DMA((4,)), pltpu.VMEM((slices, width), f32)],
        )(*(distant(a) if i > 3 and i < 8 else a for i, a in enumerate(arrays)))
    outs = [pltpu.HBM((slices, width), bf16)] * 3 + [norms]
    coil_spec = pl.BlockSpec((1,) + own.shape[1:], lambda g: (g, 0, 0))
    spectrum_spec = pl.BlockSpec((2 * group, slices, wide), lambda g: (g, 0, 0))
    return call(
        kernel,
        2 * 10**9,
        grid=(steps,),
        in_specs=[whole(image), whole(sampling), coil_spec, coil_spec, *(whole(a) for a in arrays[4:])],
        out_specs=[*(whole(o) for o in outs), spectrum_spec],
        out_shape=[*outs, pltpu.HBM((steps * 2 * group, slices, wide), bf16)],
        scratch_shapes=scratch,
    )(*arrays)


def adjoint_step(spectrum, own, other, tables, width):
    _, column_inv, depth_fwd, depth_inv = tables
    _, slices, wide = spectrum.shape
    encodings = wide // 512
    steps = own.shape[0]
    group = own.shape[2] // WIDE

    def kernel(spectrum_ref, own_ref, other_ref, wi, zf, zi, out_ref, product):
        @pl.when(pl.program_id(0) == 0)
        def _():
            out_ref[...] = jnp.zeros(out_ref.shape, f32)

        def one_step():
            for half in range(2):
                for k in range(group):
                    sa, sb, sd, st = (
                        spectrum_ref[half * group + k, :, j * 2 * LANE : (j + 1) * 2 * LANE]
                        for j in range(4)
                    )
                    close = dot(zi[...], stack(sa, sb)).astype(bf16)
                    far = dot(zf[:slices, :], stack(sd, st)).astype(bf16)
                    for e in range(encodings):
                        at = ((half * group + k) * encodings + e) * slices
                        for j, x in enumerate((close[:slices], close[slices:], far)):
                            product[at : at + slices, j * LANE : (j + 1) * LANE] = x[:, e * LANE : (e + 1) * LANE]
            q = dot(product[...], wi[...])
            sums = [[0.0, 0.0, 0.0] for _ in range(encodings)]
            for half, coil_ref in ((0, own_ref), (1, other_ref)):
                for k in range(group):
                    ca, cb, dr, di = coil_lanes(coil_ref, 0, k)
                    for e in range(encodings):
                        at = ((half * group + k) * encodings + e) * slices
                        qa, qb, qd, qt = (q[at : at + slices, j * LANE : (j + 1) * LANE] for j in range(4))
                        sums[e][0] += ca * qa + cb * qb
                        sums[e][1] += ca * qb - cb * qa
                        sums[e][2] += dr * qd - di * qt
            for e in range(encodings):
                for j in range(3):
                    at = e * WIDE + j * LANE
                    out_ref[:, at : at + LANE] += sums[e][j]

        one_step()

    arrays = [spectrum, own, other, column_inv, depth_fwd, depth_inv]
    coil_spec = pl.BlockSpec((1,) + own.shape[1:], lambda g: (g, 0, 0))
    spectrum_spec = pl.BlockSpec((2 * group, slices, wide), lambda g: (g, 0, 0))
    out = pltpu.HBM((slices, width), f32)
    return call(
        kernel,
        2 * 10**9,
        grid=(steps,),
        in_specs=[spectrum_spec, coil_spec, coil_spec, *(whole(a) for a in arrays[3:])],
        out_specs=whole(out),
        out_shape=out,
        scratch_shapes=[pltpu.VMEM((2 * group * encodings * slices, WIDE), bf16)],
    )(distant(spectrum), *arrays[1:])


def finish(norms_one, norms_two, data, sampling, slab_one, rows, last, readout):
    encodings, nrows, slices, lines = data.shape[1:]

    def kernel(norm_one, norm_two, data_ref, mask_ref, slab, keep, one, two, last_ref, out, image):
        lo = lax.axis_index("lo")
        alphas = step_length(norm_one), step_length(norm_two)
        for j, rows_ref in enumerate((keep, one, two)):
            r = jnp.where(lax.rem(lo, 2) == 0, j, nrows - 1 - j)
            for e in range(encodings):
                weight = mask_ref[e].astype(f32)
                real, imag = (-(data_ref[c, e, r].astype(f32) * weight) for c in range(2))
                a, b, d = (
                    alphas[0] * rows_ref[slices + 16 :, (2 * k + e) * LANE : (2 * k + e + 1) * LANE].astype(f32)
                    + alphas[1] * rows_ref[:slices, (2 * k + e) * LANE : (2 * k + e + 1) * LANE].astype(f32)
                    for k in range(3)
                )
                out[0, e, r, :, :LANE] = real[:, :LANE] - a
                out[1, e, r, :, :LANE] = imag[:, :LANE] - b
                out[0, e, r, :, LANE:] = real[:, LANE:] - d[:, :HALF]
                out[1, e, r, :, LANE:] = imag[:, LANE:] - swapped(d)[:, :HALF]
        for j in range(readout):
            x = lax.bitwise_xor(lo, j)
            for e in range(encodings):
                for k in range(3):
                    at = e * WIDE + k * LANE
                    if j < 3:
                        step = (keep, one, two)[j][slices : slices + 16, at : at + LANE]
                    else:
                        step = last_ref[:, at : at + LANE]
                    value = -alphas[0] * slab[x, :, at : at + LANE] - alphas[1] * step.astype(f32)[:8]
                    if k < 2:
                        image[k, e, x, :, :LANE] = value[:2]
                    else:
                        image[0, e, x, :, LANE:] = value[:2, :HALF]
                        image[1, e, x, :, LANE:] = swapped(value)[:2, :HALF]

    return call(
        kernel,
        10**7,
        in_specs=[VMEM] * 9,
        out_specs=[VMEM, VMEM],
        out_shape=[
            jax.ShapeDtypeStruct(data.shape, f32),
            jax.ShapeDtypeStruct((2, encodings, readout, 2, lines), f32),
        ],
    )(norms_one, norms_two, data, sampling, slab_one, *rows, last)


def reconstruct(kspace_data, coil_maps, sampling):
    encodings = kspace_data.shape[2]
    rows = kspace_data.shape[3]
    slices = kspace_data.shape[4]
    coils, readout, zdepth, lines = coil_maps.shape[1:]
    nhi, nlo = lax.axis_size("hi"), lax.axis_size("lo")
    nphase, ncore = lax.axis_size("phase"), lax.axis_size("enc")
    slabs = nhi * nlo
    group = coils // (nphase * ncore)
    assert (nlo, readout, rows, zdepth, lines, slices) == (4, 4, 3, 2, LANE + HALF, 2 * slabs)
    assert group * nhi == coils and nphase * ncore == nhi and ncore == 2
    column_fwd, column_inv = column_table(lines, -1.0), column_table(lines, 1.0)
    depth_fwd, depth_inv = depth_table(slices, -1.0), depth_table(slices, 1.0)
    tables = (column_fwd, column_inv, depth_fwd, depth_inv)
    sampling = sampling[0]
    data = kspace_data[:, 0]

    def round_ring(value):
        value = value.reshape(slabs, zdepth, -1)
        return lax.all_to_all(value, ("hi", "lo"), 0, 0, tiled=True).reshape(slices, -1)

    packed = depart(data, sampling, coil_maps, depth_inv, nhi, group)
    packed = round_ring(packed)
    coil_rows = coil_maps.reshape(2, slabs, rows, zdepth, lines).transpose(2, 0, 1, 3, 4)
    coil_rows = coil_rows.reshape(rows, 2, slices, lines)
    slab_one, spread = slab_gradient(packed, coil_rows, column_inv, encodings, nhi)
    one = round_ring(spread)
    own = lax.all_gather(packed[:, encodings * rows * WIDE :], "phase")
    other = lax.ppermute(own, "enc", [(i, (i + 1) % ncore) for i in range(ncore)])

    up = [(i, (i + 1) % nphase) for i in range(nphase)]
    before = lax.ppermute(one, "phase", up)
    after = lax.ppermute(one, "phase", [(j, i) for i, j in up])

    def total(norms):
        return lax.all_to_all(norms, ("lo", "phase", "enc"), 0, 0, tiled=True)

    members = nlo * nphase * ncore

    def swap(value, j):
        return lax.ppermute(value, "lo", [(i, i ^ j) for i in range(nlo)])

    *rows_one, norms, spectrum = forward_step(one, (), sampling, own, other, tables, members, False)
    norms_one = total(norms)
    normal = adjoint_step(spectrum, own, other, tables, one.shape[1])
    extra = (norms_one, before, after, normal, *rows_one)
    *rows_two, norms, last = forward_step(one, extra, sampling, own, other, tables, members, True)
    near = swap(rows_two[1], 1)
    far = swap(rows_two[2], 2)
    norms_two = total(norms)
    last = swap(last, 3)
    got = [rows_two[0], near, far]
    residual, image = finish(norms_one, norms_two, data, sampling, slab_one, got, last, readout)
    return (image[:, None], residual[:, None])


def solution(mesh):
    names = dict(mesh.shape)
    nlo = 4
    grid = Mesh(
        mesh.devices.reshape(names["pat"], names["slab"] // nlo, nlo, names["phase"], names["enc"]),
        ("pat", "hi", "lo", "phase", "enc"),
    )
    slab = ("hi", "lo")
    in_specs = (
        P("pat", "phase", "enc", slab, None, None),
        P("pat", None, None, slab, None),
        P("phase", "enc", "pat", None),
    )
    out_specs = (
        P("pat", "phase", "enc", None, slab, None),
        P("pat", "phase", "enc", slab, None, None),
    )
    return jax.shard_map(reconstruct, mesh=grid, in_specs=in_specs, out_specs=out_specs, check_vma=False)
```

```python
import math

import jax
import jax.numpy as jnp
import numpy as np
from jax import lax
from jax.experimental import pallas as pl
from jax.experimental.pallas import tpu as pltpu
from jax.sharding import Mesh
from jax.sharding import PartitionSpec as P

tv_weight = 0.15
smoothing = 0.6
f32 = jnp.float32
bf16 = jnp.bfloat16

LANE = 128
HALF = 64
WIDE = 384


def dft(length, direction):
    counter = np.arange(length)
    angle = (counter[:, None] * counter[None, :] % length).astype(np.float32) * np.float32(2.0 * math.pi / length)
    factor = np.float32(1.0 / math.sqrt(length))
    return np.cos(angle) * factor, np.float32(direction) * np.sin(angle) * factor


def column_table(length, direction):
    real, imag = dft(length, direction)
    whole = np.concatenate(
        [np.concatenate([real, imag], axis=1), np.concatenate([-imag, real], axis=1)], axis=0
    )
    order = np.concatenate(
        [
            np.arange(LANE),
            length + np.arange(LANE),
            np.arange(LANE, length),
            length + np.arange(LANE, length),
        ]
    )
    packed = whole[order][:, order]
    tail = np.concatenate([-packed[:, WIDE - HALF :], packed[:, WIDE - LANE : WIDE - HALF]], axis=1)
    return jnp.asarray(np.concatenate([packed, tail], axis=1), dtype=bf16)


def depth_table(length, direction):
    real, imag = dft(length, direction)
    return jnp.asarray(
        np.concatenate(
            [np.concatenate([real, -imag], axis=1), np.concatenate([imag, real], axis=1)], axis=0
        ),
        dtype=bf16,
    )


def dot(a, b):
    return jnp.dot(a, b, preferred_element_type=f32)


def lanes(*pieces):
    return jnp.concatenate(pieces, axis=1)


def stack(*pieces):
    return jnp.concatenate(pieces, axis=0)


def left_half(shape):
    return lax.broadcasted_iota(jnp.int32, shape, 1) < HALF


def swapped(d):
    return pltpu.roll(d, HALF, 1)


def times_i(d):
    other = swapped(d)
    return jnp.where(left_half(d.shape), -other, other)


def doubled(d):
    other = swapped(d)
    left = left_half(d.shape)
    return jnp.where(left, d, other), jnp.where(left, other, d)


def mask_lanes(mask):
    mask = mask.astype(f32)
    return mask[:, :LANE], lanes(mask[:, LANE:], mask[:, LANE:])


def call(kernel, flops, **kwargs):
    return pl.pallas_call(
        kernel,
        cost_estimate=pl.CostEstimate(flops=flops, transcendentals=0, bytes_accessed=2**20),
        compiler_params=pltpu.CompilerParams(vmem_limit_bytes=32 * 2**20),
        **kwargs,
    )


VMEM = pl.BlockSpec(memory_space=pltpu.VMEM)


def distant(value):
    return pltpu.with_memory_space_constraint(value, pltpu.HBM)


def depart(data, sampling, coils, depth_inv, nhi, group):
    encodings, rows, slices, _ = data.shape[1:]
    images = encodings * rows

    slabs = slices // 2

    def kernel(data_ref, mask_ref, coil_ref, table, out):
        share_index = lax.axis_index("phase") * lax.axis_size("enc") + lax.axis_index("enc")
        for e in range(encodings):
            weight = -mask_ref[e].astype(f32)
            for r in range(rows):
                both = stack(*((data_ref[c, e, r].astype(f32) * weight).astype(bf16) for c in range(2)))
                both = dot(table[...], both)
                real, imag = both[:slices], both[slices:]
                at = (e * rows + r) * WIDE
                for j, x in enumerate((real[:, :LANE], imag[:, :LANE], lanes(real[:, LANE:], imag[:, LANE:]))):
                    x = x.astype(bf16).reshape(slabs, 2, LANE)
                    out[:, :, at + j * LANE : at + (j + 1) * LANE] = x
        first = share_index * group
        for k in range(group):
            real, imag = (coil_ref[c, first + k].astype(f32) for c in range(2))
            tail = jnp.concatenate([real[:, :, LANE:], imag[:, :, LANE:]], axis=2)
            at = (images + k) * WIDE
            for j, x in enumerate((real[:, :, :LANE], imag[:, :, :LANE], tail)):
                x = x.astype(bf16)
                for h in range(nhi):
                    out[4 * h : 4 * h + 4, :, at + j * LANE : at + (j + 1) * LANE] = x

    return call(
        kernel,
        10**8,
        in_specs=[VMEM, VMEM, VMEM, VMEM],
        out_specs=VMEM,
        out_shape=jax.ShapeDtypeStruct((slabs, 2, (images + group) * WIDE), bf16),
    )(*(distant(a) for a in (data, sampling, coils, depth_inv)))


def slab_gradient(packed, coil_rows, column_inv, encodings, nhi, first):
    rows, _, slices, _ = coil_rows.shape

    def kernel(in_ref, coil_ref, table, out, send):
        images = [in_ref[:, i * WIDE : (i + 1) * WIDE] for i in range(encodings * rows)]
        fine = dot(stack(*images), table[...])
        coil = []
        for r in range(rows):
            real, imag = coil_ref[r, 0].astype(f32), coil_ref[r, 1].astype(f32)
            coil.append(
                (
                    real[:, :LANE],
                    imag[:, :LANE],
                    lanes(real[:, LANE:], real[:, LANE:]),
                    lanes(imag[:, LANE:], imag[:, LANE:]),
                )
            )
        even = lax.rem(lax.broadcasted_iota(jnp.int32, (8, WIDE), 0) // 2, 2) == 0
        for e in range(encodings):
            total = jnp.zeros((8, WIDE), f32)
            for r in range(rows):
                at = (e * rows + r) * slices
                a, b, d, t = (fine[at : at + slices, j * LANE : (j + 1) * LANE] for j in range(4))
                ca, cb, dr, di = coil[r]
                value = lanes(ca * a + cb * b, ca * b - cb * a, dr * d - di * t)
                value = jnp.sum(value.reshape(slices // 8, 8, WIDE), axis=0)
                turned = (-2 * r) % 8
                one = value if turned == 0 else pltpu.roll(value, turned, 0)
                two = pltpu.roll(value, (turned + 4) % 8, 0) if (turned + 4) % 8 else value
                total = total + jnp.where(even, one, two)
            for x in range(4):
                mine = pltpu.roll(total, 8 - 2 * x, 0) if x else total
                out[x, :, e * WIDE : (e + 1) * WIDE] = mine
                for h in range(nhi):
                    send[(4 * h + x - first) % (4 * nhi), :, e * WIDE : (e + 1) * WIDE] = mine[:2].astype(bf16)

    return call(
        kernel,
        10**8,
        in_specs=[VMEM, VMEM, VMEM],
        out_specs=[VMEM, VMEM],
        out_shape=[
            jax.ShapeDtypeStruct((4, 8, encodings * WIDE), f32),
            jax.ShapeDtypeStruct((slices // 2, 2, encodings * WIDE), bf16),
        ],
    )(packed, coil_rows, column_inv)


def step_length(norm_ref):
    gg, ee = (jnp.sum(norm_ref[:, i : i + 1, :], axis=0) for i in range(2))
    return gg / (ee + 4.0 * tv_weight / smoothing * gg + 1e-06)


def whole(array):
    return pl.BlockSpec(array.shape, lambda g, _n=len(array.shape): (0,) * _n)


def coil_lanes(ref, step, k):
    a, b, d = (ref[step, :, k * WIDE + j * LANE : k * WIDE + (j + 1) * LANE].astype(f32) for j in range(3))
    return (a, b, *doubled(d))


def forward_step(image, extra, sampling, own, other, tables, members, second):
    column_fwd, _, depth_fwd, depth_inv = tables
    slices, width = image.shape
    encodings = width // WIDE
    steps = own.shape[0]
    group = own.shape[2] // WIDE
    nlo = 4

    def kernel(*refs):
        refs = list(refs)
        if second:
            norms_ref, image_ref, before_ref, after_ref, normal_ref, *firsts = (refs.pop(0) for _ in range(8))
        else:
            image_ref = refs.pop(0)
        mask_ref, own_ref, other_ref, wf, zf, zi = (refs.pop(0) for _ in range(6))
        sends = [refs.pop(0) for _ in range(3)]
        norm_ref, out_ref = refs.pop(0), refs.pop(0)
        value, ahead_ref, mask_a, mask_d, product, squares, *spectra = refs
        spectrum = spectra[0] if second else out_ref
        copies = []
        if second:
            for j in range(3):
                copies.append(
                    pltpu.make_async_copy(firsts[j], sends[j].at[pl.ds(slices + 16, slices)], spectra[1].at[j])
                )
            copies.append(pltpu.make_async_copy(normal_ref, spectra[2], spectra[1].at[3]))
            for copy in reversed(copies):
                copy.start()
        only = lambda condition: (lambda f: f()) if second else pl.when(condition)
        hi, lo, core = (lax.axis_index(name) for name in ("hi", "lo", "enc"))

        def column(ref, e, j):
            at = e * WIDE + j * LANE
            return ref[:, at : at + LANE].astype(f32)

        @only(pl.program_id(0) == 0 if not second else True)
        def _():
            total = jnp.zeros((slices, LANE), f32)
            for e in range(encodings):
                now = [column(image_ref, e, j) for j in range(3)]
                if second:
                    alpha = step_length(norms_ref)
                    new = [-alpha * v for v in now]
                    slopes = []
                    for d in (
                        [new[j] + alpha * column(before_ref, e, j) for j in range(3)],
                        [-alpha * column(after_ref, e, j) - new[j] for j in range(3)],
                    ):
                        close = jnp.sqrt(d[0] * d[0] + d[1] * d[1] + smoothing * smoothing)
                        square = d[2] * d[2]
                        far = jnp.sqrt(square + swapped(square) + smoothing * smoothing)
                        slopes.append([d[0] / close, d[1] / close, d[2] / far])
                    now = [now[j] + tv_weight * (slopes[0][j] - slopes[1][j]) for j in range(3)]
                    for j in range(3):
                        at = e * WIDE + j * LANE
                        ahead_ref[:, at : at + LANE] = now[j]
            if second:
                copies[3].wait()
            for e in range(encodings):
                now = [column(image_ref, e, j) for j in range(3)]
                if second:
                    now = [column(ahead_ref, e, j) - alpha * column(spectra[2], e, j) for j in range(3)]
                    for j in range(3):
                        at = e * WIDE + j * LANE
                        ahead_ref[:, at : at + LANE] = now[j]
                for j in range(3):
                    total = total + now[j] * now[j]
                    now[j] = now[j].astype(bf16).astype(f32)
                    value[:, e * 512 + j * LANE : e * 512 + (j + 1) * LANE] = now[j]
                value[:, e * 512 + 3 * LANE : (e + 1) * 512] = times_i(now[2])
                a, d = mask_lanes(mask_ref[e])
                mask_a[:, e * LANE : (e + 1) * LANE] = a
                mask_d[:, e * LANE : (e + 1) * LANE] = d
            norm_ref[:, 0:1, :] = jnp.full((members, 1, LANE), jnp.sum(total), f32)
            squares[...] = jnp.zeros(squares.shape, f32)

        def one_step(step, carry):
            at_step = step if second else 0
            for half, coil_ref in ((0, own_ref), (1, other_ref)):
                for k in range(group):
                    ca, cb, dr, di = coil_lanes(coil_ref, at_step, k)
                    for e in range(encodings):
                        va, vb, vd, vt = (value[:, e * 512 + j * LANE : e * 512 + (j + 1) * LANE] for j in range(4))
                        at = ((half * group + k) * encodings + e) * slices
                        product[at : at + slices, :LANE] = (ca * va - cb * vb).astype(bf16)
                        product[at : at + slices, LANE : 2 * LANE] = (ca * vb + cb * va).astype(bf16)
                        product[at : at + slices, 2 * LANE :] = (dr * vd + di * vt).astype(bf16)
            weight_a, weight_d = mask_a[...], mask_d[...]
            total = jnp.zeros(weight_a.shape, f32)
            u = dot(product[...], wf[...]).astype(bf16)
            for k in range(2 * group):

                def pair(j):
                    return lanes(
                        *(
                            u[(k * encodings + e) * slices : (k * encodings + e + 1) * slices, j * LANE : (j + 1) * LANE]
                            for e in range(encodings)
                        )
                    )

                close = dot(zf[...], stack(pair(0), pair(1)))
                sd = dot(zi[:slices, :], stack(pair(2), pair(3))) * weight_d
                sa, sb = close[:slices] * weight_a, close[slices:] * weight_a
                total = total + (sa * sa + sb * sb + sd * sd)
                parts = [sa, sb, sd]
                if not second:
                    parts.append(lanes(*(times_i(sd[:, e * LANE : (e + 1) * LANE]) for e in range(encodings))))
                for j, x in enumerate(parts):
                    spectrum[k, :, j * 2 * LANE : (j + 1) * 2 * LANE] = x.astype(bf16)
            squares[...] += total
            for half in range(2):
                owner = 2 * step + (core if half == 0 else 1 - core)

                @pl.when(owner == hi)
                def _():
                    for j, send_ref in enumerate(sends):
                        dest = lax.bitwise_xor(lo, j)
                        coil = (3 * dest + lax.rem(lo + dest, nlo)) // nlo
                        send_ref[:slices] = spectrum[half * group + coil, :, :width]

            return carry

        if second:
            lax.fori_loop(0, steps, one_step, 0)
        else:
            one_step(pl.program_id(0), 0)
        if second:
            piece = ahead_ref[pl.ds(pl.multiple_of(8 * hi, 8), 8), :]
            turned = [pltpu.roll(piece, 8 - 2 * dest, 0) if dest else piece for dest in range(nlo)]
            for j in range(nlo):
                dest = lax.bitwise_xor(lo, j)
                part = turned[0]
                for k in range(1, nlo):
                    part = jnp.where(dest == k, turned[k], part)
                part = stack(part, part).astype(bf16)
                if j < 3:
                    sends[j][slices : slices + 16] = part
                    copies[j].wait()
                else:
                    out_ref[...] = part

        @only(pl.program_id(0) == steps - 1 if not second else True)
        def _():
            norm_ref[:, 1:2, :] = jnp.full((members, 1, LANE), jnp.sum(squares[...]), f32)

    arrays = [*extra[:1], image, *extra[1:], sampling, own, other, column_fwd, depth_fwd, depth_inv]
    wide = encodings * 512
    norms = jax.ShapeDtypeStruct((members, 2, LANE), f32)
    scratch = [
        pltpu.VMEM((slices, wide), f32),
        pltpu.VMEM((slices, width), f32),
        pltpu.VMEM((slices, encodings * LANE), f32),
        pltpu.VMEM((slices, encodings * LANE), f32),
        pltpu.VMEM((2 * group * encodings * slices, WIDE), bf16),
        pltpu.VMEM((slices, encodings * LANE), f32),
    ]
    if second:
        outs = [jax.ShapeDtypeStruct((2 * slices + 16, width), bf16)] * 3
        return call(
            kernel,
            2 * 10**9,
            in_specs=[VMEM] * 4 + [pl.BlockSpec(memory_space=pl.ANY)] * 4 + [VMEM] * (len(arrays) - 8),
            out_specs=[VMEM] * 5,
            out_shape=[*outs, norms, jax.ShapeDtypeStruct((16, width), bf16)],
            scratch_shapes=[*scratch, pltpu.VMEM((2 * group, slices, width), bf16), pltpu.SemaphoreType.DMA((4,)), pltpu.VMEM((slices, width), f32)],
        )(*(distant(a) if i > 3 and i < 8 else a for i, a in enumerate(arrays)))
    outs = [pltpu.HBM((slices, width), bf16)] * 3 + [norms]
    coil_spec = pl.BlockSpec((1,) + own.shape[1:], lambda g: (g, 0, 0))
    spectrum_spec = pl.BlockSpec((2 * group, slices, wide), lambda g: (g, 0, 0))
    return call(
        kernel,
        2 * 10**9,
        grid=(steps,),
        in_specs=[whole(image), whole(sampling), coil_spec, coil_spec, *(whole(a) for a in arrays[4:])],
        out_specs=[*(whole(o) for o in outs), spectrum_spec],
        out_shape=[*outs, pltpu.HBM((steps * 2 * group, slices, wide), bf16)],
        scratch_shapes=scratch,
    )(*arrays)


def adjoint_step(spectrum, own, other, tables, width):
    _, column_inv, depth_fwd, depth_inv = tables
    _, slices, wide = spectrum.shape
    encodings = wide // 512
    steps = own.shape[0]
    group = own.shape[2] // WIDE

    def kernel(spectrum_ref, own_ref, other_ref, wi, zf, zi, out_ref, product):
        @pl.when(pl.program_id(0) == 0)
        def _():
            out_ref[...] = jnp.zeros(out_ref.shape, f32)

        def one_step():
            for half in range(2):
                for k in range(group):
                    sa, sb, sd, st = (
                        spectrum_ref[half * group + k, :, j * 2 * LANE : (j + 1) * 2 * LANE]
                        for j in range(4)
                    )
                    close = dot(zi[...], stack(sa, sb)).astype(bf16)
                    far = dot(zf[:slices, :], stack(sd, st)).astype(bf16)
                    for e in range(encodings):
                        at = ((half * group + k) * encodings + e) * slices
                        for j, x in enumerate((close[:slices], close[slices:], far)):
                            product[at : at + slices, j * LANE : (j + 1) * LANE] = x[:, e * LANE : (e + 1) * LANE]
            q = dot(product[...], wi[...])
            sums = [[0.0, 0.0, 0.0] for _ in range(encodings)]
            for half, coil_ref in ((0, own_ref), (1, other_ref)):
                for k in range(group):
                    ca, cb, dr, di = coil_lanes(coil_ref, 0, k)
                    for e in range(encodings):
                        at = ((half * group + k) * encodings + e) * slices
                        qa, qb, qd, qt = (q[at : at + slices, j * LANE : (j + 1) * LANE] for j in range(4))
                        sums[e][0] += ca * qa + cb * qb
                        sums[e][1] += ca * qb - cb * qa
                        sums[e][2] += dr * qd - di * qt
            for e in range(encodings):
                for j in range(3):
                    at = e * WIDE + j * LANE
                    out_ref[:, at : at + LANE] += sums[e][j]

        one_step()

    arrays = [spectrum, own, other, column_inv, depth_fwd, depth_inv]
    coil_spec = pl.BlockSpec((1,) + own.shape[1:], lambda g: (g, 0, 0))
    spectrum_spec = pl.BlockSpec((2 * group, slices, wide), lambda g: (g, 0, 0))
    out = pltpu.HBM((slices, width), f32)
    return call(
        kernel,
        2 * 10**9,
        grid=(steps,),
        in_specs=[spectrum_spec, coil_spec, coil_spec, *(whole(a) for a in arrays[3:])],
        out_specs=whole(out),
        out_shape=out,
        scratch_shapes=[pltpu.VMEM((2 * group * encodings * slices, WIDE), bf16)],
    )(distant(spectrum), *arrays[1:])


def finish(norms_one, norms_two, data, sampling, slab_one, rows, last, readout):
    encodings, nrows, slices, lines = data.shape[1:]

    def kernel(norm_one, norm_two, data_ref, mask_ref, slab, keep, one, two, last_ref, out, image):
        lo = lax.axis_index("lo")
        alphas = step_length(norm_one), step_length(norm_two)
        for j, rows_ref in enumerate((keep, one, two)):
            r = jnp.where(lax.rem(lo, 2) == 0, j, nrows - 1 - j)
            for e in range(encodings):
                weight = mask_ref[e].astype(f32)
                real, imag = (-(data_ref[c, e, r].astype(f32) * weight) for c in range(2))
                a, b, d = (
                    alphas[0] * rows_ref[slices + 16 :, (2 * k + e) * LANE : (2 * k + e + 1) * LANE].astype(f32)
                    + alphas[1] * rows_ref[:slices, (2 * k + e) * LANE : (2 * k + e + 1) * LANE].astype(f32)
                    for k in range(3)
                )
                out[0, e, r, :, :LANE] = real[:, :LANE] - a
                out[1, e, r, :, :LANE] = imag[:, :LANE] - b
                out[0, e, r, :, LANE:] = real[:, LANE:] - d[:, :HALF]
                out[1, e, r, :, LANE:] = imag[:, LANE:] - swapped(d)[:, :HALF]
        for j in range(readout):
            x = lax.bitwise_xor(lo, j)
            for e in range(encodings):
                for k in range(3):
                    at = e * WIDE + k * LANE
                    if j < 3:
                        step = (keep, one, two)[j][slices : slices + 16, at : at + LANE]
                    else:
                        step = last_ref[:, at : at + LANE]
                    value = -alphas[0] * slab[x, :, at : at + LANE] - alphas[1] * step.astype(f32)[:8]
                    if k < 2:
                        image[k, e, x, :, :LANE] = value[:2]
                    else:
                        image[0, e, x, :, LANE:] = value[:2, :HALF]
                        image[1, e, x, :, LANE:] = swapped(value)[:2, :HALF]

    return call(
        kernel,
        10**7,
        in_specs=[VMEM] * 9,
        out_specs=[VMEM, VMEM],
        out_shape=[
            jax.ShapeDtypeStruct(data.shape, f32),
            jax.ShapeDtypeStruct((2, encodings, readout, 2, lines), f32),
        ],
    )(norms_one, norms_two, data, sampling, slab_one, *rows, last)


def reconstruct(kspace_data, coil_maps, sampling):
    encodings = kspace_data.shape[2]
    rows = kspace_data.shape[3]
    slices = kspace_data.shape[4]
    coils, readout, zdepth, lines = coil_maps.shape[1:]
    nhi, nlo = lax.axis_size("hi"), lax.axis_size("lo")
    nphase, ncore = lax.axis_size("phase"), lax.axis_size("enc")
    slabs = nhi * nlo
    group = coils // (nphase * ncore)
    assert (nlo, readout, rows, zdepth, lines, slices) == (4, 4, 3, 2, LANE + HALF, 2 * slabs)
    assert group * nhi == coils and nphase * ncore == nhi and ncore == 2
    column_fwd, column_inv = column_table(lines, -1.0), column_table(lines, 1.0)
    depth_fwd, depth_inv = depth_table(slices, -1.0), depth_table(slices, 1.0)
    tables = (column_fwd, column_inv, depth_fwd, depth_inv)
    sampling = sampling[0]
    data = kspace_data[:, 0]

    def round_ring(value):
        value = value.reshape(slabs, zdepth, -1)
        return lax.all_to_all(value, ("hi", "lo"), 0, 0, tiled=True).reshape(slices, -1)

    packed = depart(data, sampling, coil_maps, depth_inv, nhi, group)
    packed = round_ring(packed)
    coil_rows = coil_maps.reshape(2, slabs, rows, zdepth, lines).transpose(2, 0, 1, 3, 4)
    coil_rows = coil_rows.reshape(rows, 2, slices, lines)
    first = nlo + nlo // 2
    slab_one, spread = slab_gradient(packed, coil_rows, column_inv, encodings, nhi, first)
    order = [(i + first) % slabs for i in range(slabs)]
    one = lax.all_to_all(spread, ("hi", "lo"), 0, 0, tiled=True, axis_index_groups=[order])
    one = jnp.roll(one, first, axis=0).reshape(slices, -1)
    own = lax.all_gather(packed[:, encodings * rows * WIDE :], "phase")
    other = lax.ppermute(own, "enc", [(i, (i + 1) % ncore) for i in range(ncore)])

    up = [(i, (i + 1) % nphase) for i in range(nphase)]
    before = lax.ppermute(one, "phase", up)
    after = lax.ppermute(one, "phase", [(j, i) for i, j in up])

    def total(norms):
        return lax.all_to_all(norms, ("lo", "phase", "enc"), 0, 0, tiled=True)

    members = nlo * nphase * ncore

    def swap(value, j):
        return lax.ppermute(value, "lo", [(i, i ^ j) for i in range(nlo)])

    *rows_one, norms, spectrum = forward_step(one, (), sampling, own, other, tables, members, False)
    norms_one = total(norms)
    normal = adjoint_step(spectrum, own, other, tables, one.shape[1])
    extra = (norms_one, before, after, normal, *rows_one)
    *rows_two, norms, last = forward_step(one, extra, sampling, own, other, tables, members, True)
    near = swap(rows_two[1], 1)
    far = swap(rows_two[2], 2)
    norms_two = total(norms)
    last = swap(last, 3)
    got = [rows_two[0], near, far]
    residual, image = finish(norms_one, norms_two, data, sampling, slab_one, got, last, readout)
    return (image[:, None], residual[:, None])


def solution(mesh):
    names = dict(mesh.shape)
    nlo = 4
    grid = Mesh(
        mesh.devices.reshape(names["pat"], names["slab"] // nlo, nlo, names["phase"], names["enc"]),
        ("pat", "hi", "lo", "phase", "enc"),
    )
    slab = ("hi", "lo")
    in_specs = (
        P("pat", "phase", "enc", slab, None, None),
        P("pat", None, None, slab, None),
        P("phase", "enc", "pat", None),
    )
    out_specs = (
        P("pat", "phase", "enc", None, slab, None),
        P("pat", "phase", "enc", slab, None, None),
    )
    return jax.shard_map(reconstruct, mesh=grid, in_specs=in_specs, out_specs=out_specs, check_vma=False)
```

```python
import math

import jax
import jax.numpy as jnp
import numpy as np
from jax import lax
from jax.experimental import pallas as pl
from jax.experimental.pallas import tpu as pltpu
from jax.sharding import Mesh
from jax.sharding import PartitionSpec as P

tv_weight = 0.15
smoothing = 0.6
f32 = jnp.float32
bf16 = jnp.bfloat16

LANE = 128
HALF = 64
WIDE = 384


def dft(length, direction):
    counter = np.arange(length)
    angle = (counter[:, None] * counter[None, :] % length).astype(np.float32) * np.float32(2.0 * math.pi / length)
    factor = np.float32(1.0 / math.sqrt(length))
    return np.cos(angle) * factor, np.float32(direction) * np.sin(angle) * factor


def column_table(length, direction):
    real, imag = dft(length, direction)
    whole = np.concatenate(
        [np.concatenate([real, imag], axis=1), np.concatenate([-imag, real], axis=1)], axis=0
    )
    order = np.concatenate(
        [
            np.arange(LANE),
            length + np.arange(LANE),
            np.arange(LANE, length),
            length + np.arange(LANE, length),
        ]
    )
    packed = whole[order][:, order]
    tail = np.concatenate([-packed[:, WIDE - HALF :], packed[:, WIDE - LANE : WIDE - HALF]], axis=1)
    return jnp.asarray(np.concatenate([packed, tail], axis=1), dtype=bf16)


def depth_table(length, direction):
    real, imag = dft(length, direction)
    return jnp.asarray(
        np.concatenate(
            [np.concatenate([real, -imag], axis=1), np.concatenate([imag, real], axis=1)], axis=0
        ),
        dtype=bf16,
    )


def dot(a, b):
    return jnp.dot(a, b, preferred_element_type=f32)


def lanes(*pieces):
    return jnp.concatenate(pieces, axis=1)


def stack(*pieces):
    return jnp.concatenate(pieces, axis=0)


def left_half(shape):
    return lax.broadcasted_iota(jnp.int32, shape, 1) < HALF


def swapped(d):
    return pltpu.roll(d, HALF, 1)


def times_i(d):
    other = swapped(d)
    return jnp.where(left_half(d.shape), -other, other)


def doubled(d):
    other = swapped(d)
    left = left_half(d.shape)
    return jnp.where(left, d, other), jnp.where(left, other, d)


def mask_lanes(mask):
    mask = mask.astype(f32)
    return mask[:, :LANE], lanes(mask[:, LANE:], mask[:, LANE:])


def call(kernel, flops, **kwargs):
    return pl.pallas_call(
        kernel,
        cost_estimate=pl.CostEstimate(flops=flops, transcendentals=0, bytes_accessed=2**20),
        compiler_params=pltpu.CompilerParams(vmem_limit_bytes=32 * 2**20),
        **kwargs,
    )


VMEM = pl.BlockSpec(memory_space=pltpu.VMEM)


def distant(value):
    return pltpu.with_memory_space_constraint(value, pltpu.HBM)


def depart(data, sampling, coils, depth_inv, nhi, group):
    encodings, rows, slices, _ = data.shape[1:]
    images = encodings * rows

    slabs = slices // 2

    def kernel(data_ref, mask_ref, coil_ref, table, out):
        share_index = lax.axis_index("phase") * lax.axis_size("enc") + lax.axis_index("enc")
        step = pl.program_id(0)

        @pl.when(step < encodings)
        def _():
            weight = -mask_ref[0].astype(f32)
            for r in range(rows):
                both = stack(*((data_ref[c, 0, r].astype(f32) * weight).astype(bf16) for c in range(2)))
                both = dot(table[...], both)
                real, imag = both[:slices], both[slices:]
                at = r * WIDE
                for j, x in enumerate((real[:, :LANE], imag[:, :LANE], lanes(real[:, LANE:], imag[:, LANE:]))):
                    x = x.astype(bf16).reshape(slabs, 2, LANE)
                    out[:, :, at + j * LANE : at + (j + 1) * LANE] = x

        @pl.when(step == encodings)
        def _():
            first = share_index * group
            for k in range(group):
                real, imag = (coil_ref[c, first + k].astype(f32) for c in range(2))
                tail = jnp.concatenate([real[:, :, LANE:], imag[:, :, LANE:]], axis=2)
                at = k * WIDE
                for j, x in enumerate((real[:, :, :LANE], imag[:, :, :LANE], tail)):
                    x = x.astype(bf16)
                    for h in range(nhi):
                        out[4 * h : 4 * h + 4, :, at + j * LANE : at + (j + 1) * LANE] = x

    return call(
        kernel,
        10**8,
        grid=(encodings + 1,),
        in_specs=[
            pl.BlockSpec((2, 1, *data.shape[2:]), lambda g: (0, jnp.minimum(g, encodings - 1), 0, 0, 0)),
            pl.BlockSpec((1, *sampling.shape[1:]), lambda g: (jnp.minimum(g, encodings - 1), 0, 0)),
            whole(coils),
            whole(depth_inv),
        ],
        out_specs=pl.BlockSpec((slabs, 2, rows * WIDE), lambda g: (0, 0, g)),
        out_shape=jax.ShapeDtypeStruct((slabs, 2, (images + group) * WIDE), bf16),
    )(*(distant(a) for a in (data, sampling, coils, depth_inv)))


def slab_gradient(packed, coil_rows, column_inv, encodings, nhi):
    rows, _, slices, _ = coil_rows.shape

    def kernel(in_ref, coil_ref, table, out, send):
        images = [in_ref[:, i * WIDE : (i + 1) * WIDE] for i in range(encodings * rows)]
        fine = dot(stack(*images), table[...])
        coil = []
        for r in range(rows):
            real, imag = coil_ref[r, 0].astype(f32), coil_ref[r, 1].astype(f32)
            coil.append(
                (
                    real[:, :LANE],
                    imag[:, :LANE],
                    lanes(real[:, LANE:], real[:, LANE:]),
                    lanes(imag[:, LANE:], imag[:, LANE:]),
                )
            )
        even = lax.rem(lax.broadcasted_iota(jnp.int32, (8, WIDE), 0) // 2, 2) == 0
        for e in range(encodings):
            total = jnp.zeros((8, WIDE), f32)
            for r in range(rows):
                at = (e * rows + r) * slices
                a, b, d, t = (fine[at : at + slices, j * LANE : (j + 1) * LANE] for j in range(4))
                ca, cb, dr, di = coil[r]
                value = lanes(ca * a + cb * b, ca * b - cb * a, dr * d - di * t)
                value = jnp.sum(value.reshape(slices // 8, 8, WIDE), axis=0)
                turned = (-2 * r) % 8
                one = value if turned == 0 else pltpu.roll(value, turned, 0)
                two = pltpu.roll(value, (turned + 4) % 8, 0) if (turned + 4) % 8 else value
                total = total + jnp.where(even, one, two)
            for x in range(4):
                mine = pltpu.roll(total, 8 - 2 * x, 0) if x else total
                out[x, :, e * WIDE : (e + 1) * WIDE] = mine
                for h in range(nhi):
                    send[4 * h + x, :, e * WIDE : (e + 1) * WIDE] = mine[:2].astype(bf16)

    return call(
        kernel,
        10**8,
        in_specs=[VMEM, VMEM, VMEM],
        out_specs=[VMEM, VMEM],
        out_shape=[
            jax.ShapeDtypeStruct((4, 8, encodings * WIDE), f32),
            jax.ShapeDtypeStruct((slices // 2, 2, encodings * WIDE), bf16),
        ],
    )(packed, coil_rows, column_inv)


def step_length(norm_ref):
    gg, ee = (jnp.sum(norm_ref[:, i : i + 1, :], axis=0) for i in range(2))
    return gg / (ee + 4.0 * tv_weight / smoothing * gg + 1e-06)


def whole(array):
    return pl.BlockSpec(array.shape, lambda g, _n=len(array.shape): (0,) * _n)


def coil_lanes(ref, step, k):
    a, b, d = (ref[step, :, k * WIDE + j * LANE : k * WIDE + (j + 1) * LANE].astype(f32) for j in range(3))
    return (a, b, *doubled(d))


def forward_step(image, extra, sampling, own, other, tables, members, second):
    column_fwd, _, depth_fwd, depth_inv = tables
    slices, width = image.shape
    encodings = width // WIDE
    steps = own.shape[0]
    group = own.shape[2] // WIDE
    nlo = 4

    def kernel(*refs):
        refs = list(refs)
        if second:
            norms_ref, image_ref, before_ref, after_ref, normal_ref, *firsts = (refs.pop(0) for _ in range(8))
        else:
            image_ref = refs.pop(0)
        mask_ref, own_ref, other_ref, wf, zf, zi = (refs.pop(0) for _ in range(6))
        sends = [refs.pop(0) for _ in range(3)]
        norm_ref, out_ref = refs.pop(0), refs.pop(0)
        value, ahead_ref, mask_a, mask_d, product, squares, *spectra = refs
        spectrum = spectra[0] if second else out_ref
        copies = []
        if second:
            for j in range(3):
                copies.append(
                    pltpu.make_async_copy(firsts[j], sends[j].at[pl.ds(slices + 16, slices)], spectra[1].at[j])
                )
            copies.append(pltpu.make_async_copy(normal_ref, spectra[2], spectra[1].at[3]))
            for copy in reversed(copies):
                copy.start()
        only = lambda condition: (lambda f: f()) if second else pl.when(condition)
        hi, lo, core = (lax.axis_index(name) for name in ("hi", "lo", "enc"))

        def column(ref, e, j):
            at = e * WIDE + j * LANE
            return ref[:, at : at + LANE].astype(f32)

        @only(pl.program_id(0) == 0 if not second else True)
        def _():
            total = jnp.zeros((slices, LANE), f32)
            for e in range(encodings):
                now = [column(image_ref, e, j) for j in range(3)]
                if second:
                    alpha = step_length(norms_ref)
                    new = [-alpha * v for v in now]
                    slopes = []
                    for d in (
                        [new[j] + alpha * column(before_ref, e, j) for j in range(3)],
                        [-alpha * column(after_ref, e, j) - new[j] for j in range(3)],
                    ):
                        close = jnp.sqrt(d[0] * d[0] + d[1] * d[1] + smoothing * smoothing)
                        square = d[2] * d[2]
                        far = jnp.sqrt(square + swapped(square) + smoothing * smoothing)
                        slopes.append([d[0] / close, d[1] / close, d[2] / far])
                    now = [now[j] + tv_weight * (slopes[0][j] - slopes[1][j]) for j in range(3)]
                    for j in range(3):
                        at = e * WIDE + j * LANE
                        ahead_ref[:, at : at + LANE] = now[j]
            if second:
                copies[3].wait()
            for e in range(encodings):
                now = [column(image_ref, e, j) for j in range(3)]
                if second:
                    now = [column(ahead_ref, e, j) - alpha * column(spectra[2], e, j) for j in range(3)]
                    for j in range(3):
                        at = e * WIDE + j * LANE
                        ahead_ref[:, at : at + LANE] = now[j]
                for j in range(3):
                    total = total + now[j] * now[j]
                    now[j] = now[j].astype(bf16).astype(f32)
                    value[:, e * 512 + j * LANE : e * 512 + (j + 1) * LANE] = now[j]
                value[:, e * 512 + 3 * LANE : (e + 1) * 512] = times_i(now[2])
                a, d = mask_lanes(mask_ref[e])
                mask_a[:, e * LANE : (e + 1) * LANE] = a
                mask_d[:, e * LANE : (e + 1) * LANE] = d
            norm_ref[:, 0:1, :] = jnp.full((members, 1, LANE), jnp.sum(total), f32)
            squares[...] = jnp.zeros(squares.shape, f32)

        def one_step(step, carry):
            at_step = step if second else 0
            for half, coil_ref in ((0, own_ref), (1, other_ref)):
                for k in range(group):
                    ca, cb, dr, di = coil_lanes(coil_ref, at_step, k)
                    for e in range(encodings):
                        va, vb, vd, vt = (value[:, e * 512 + j * LANE : e * 512 + (j + 1) * LANE] for j in range(4))
                        at = ((half * group + k) * encodings + e) * slices
                        product[at : at + slices, :LANE] = (ca * va - cb * vb).astype(bf16)
                        product[at : at + slices, LANE : 2 * LANE] = (ca * vb + cb * va).astype(bf16)
                        product[at : at + slices, 2 * LANE :] = (dr * vd + di * vt).astype(bf16)
            weight_a, weight_d = mask_a[...], mask_d[...]
            total = jnp.zeros(weight_a.shape, f32)
            u = dot(product[...], wf[...]).astype(bf16)
            for k in range(2 * group):

                def pair(j):
                    return lanes(
                        *(
                            u[(k * encodings + e) * slices : (k * encodings + e + 1) * slices, j * LANE : (j + 1) * LANE]
                            for e in range(encodings)
                        )
                    )

                close = dot(zf[...], stack(pair(0), pair(1)))
                sd = dot(zi[:slices, :], stack(pair(2), pair(3))) * weight_d
                sa, sb = close[:slices] * weight_a, close[slices:] * weight_a
                total = total + (sa * sa + sb * sb + sd * sd)
                parts = [sa, sb, sd]
                if not second:
                    parts.append(lanes(*(times_i(sd[:, e * LANE : (e + 1) * LANE]) for e in range(encodings))))
                for j, x in enumerate(parts):
                    spectrum[k, :, j * 2 * LANE : (j + 1) * 2 * LANE] = x.astype(bf16)
            squares[...] += total
            for half in range(2):
                owner = 2 * step + (core if half == 0 else 1 - core)

                @pl.when(owner == hi)
                def _():
                    for j, send_ref in enumerate(sends):
                        dest = lax.bitwise_xor(lo, j)
                        coil = (3 * dest + lax.rem(lo + dest, nlo)) // nlo
                        send_ref[:slices] = spectrum[half * group + coil, :, :width]

            return carry

        if second:
            lax.fori_loop(0, steps, one_step, 0)
        else:
            one_step(pl.program_id(0), 0)
        if second:
            piece = ahead_ref[pl.ds(pl.multiple_of(8 * hi, 8), 8), :]
            turned = [pltpu.roll(piece, 8 - 2 * dest, 0) if dest else piece for dest in range(nlo)]
            for j in range(nlo):
                dest = lax.bitwise_xor(lo, j)
                part = turned[0]
                for k in range(1, nlo):
                    part = jnp.where(dest == k, turned[k], part)
                part = stack(part, part).astype(bf16)
                if j < 3:
                    sends[j][slices : slices + 16] = part
                    copies[j].wait()
                else:
                    out_ref[...] = part

        @only(pl.program_id(0) == steps - 1 if not second else True)
        def _():
            norm_ref[:, 1:2, :] = jnp.full((members, 1, LANE), jnp.sum(squares[...]), f32)

    arrays = [*extra[:1], image, *extra[1:], sampling, own, other, column_fwd, depth_fwd, depth_inv]
    wide = encodings * 512
    norms = jax.ShapeDtypeStruct((members, 2, LANE), f32)
    scratch = [
        pltpu.VMEM((slices, wide), f32),
        pltpu.VMEM((slices, width), f32),
        pltpu.VMEM((slices, encodings * LANE), f32),
        pltpu.VMEM((slices, encodings * LANE), f32),
        pltpu.VMEM((2 * group * encodings * slices, WIDE), bf16),
        pltpu.VMEM((slices, encodings * LANE), f32),
    ]
    if second:
        outs = [jax.ShapeDtypeStruct((2 * slices + 16, width), bf16)] * 3
        return call(
            kernel,
            2 * 10**9,
            in_specs=[VMEM] * 4 + [pl.BlockSpec(memory_space=pl.ANY)] * 4 + [VMEM] * (len(arrays) - 8),
            out_specs=[VMEM] * 5,
            out_shape=[*outs, norms, jax.ShapeDtypeStruct((16, width), bf16)],
            scratch_shapes=[*scratch, pltpu.VMEM((2 * group, slices, width), bf16), pltpu.SemaphoreType.DMA((4,)), pltpu.VMEM((slices, width), f32)],
        )(*(distant(a) if i > 3 and i < 8 else a for i, a in enumerate(arrays)))
    outs = [pltpu.HBM((slices, width), bf16)] * 3 + [norms]
    coil_spec = pl.BlockSpec((1,) + own.shape[1:], lambda g: (g, 0, 0))
    spectrum_spec = pl.BlockSpec((2 * group, slices, wide), lambda g: (g, 0, 0))
    return call(
        kernel,
        2 * 10**9,
        grid=(steps,),
        in_specs=[whole(image), whole(sampling), coil_spec, coil_spec, *(whole(a) for a in arrays[4:])],
        out_specs=[*(whole(o) for o in outs), spectrum_spec],
        out_shape=[*outs, pltpu.HBM((steps * 2 * group, slices, wide), bf16)],
        scratch_shapes=scratch,
    )(*arrays)


def adjoint_step(spectrum, own, other, tables, width):
    _, column_inv, depth_fwd, depth_inv = tables
    _, slices, wide = spectrum.shape
    encodings = wide // 512
    steps = own.shape[0]
    group = own.shape[2] // WIDE

    def kernel(spectrum_ref, own_ref, other_ref, wi, zf, zi, out_ref, product):
        @pl.when(pl.program_id(0) == 0)
        def _():
            out_ref[...] = jnp.zeros(out_ref.shape, f32)

        def one_step():
            for half in range(2):
                for k in range(group):
                    sa, sb, sd, st = (
                        spectrum_ref[half * group + k, :, j * 2 * LANE : (j + 1) * 2 * LANE]
                        for j in range(4)
                    )
                    close = dot(zi[...], stack(sa, sb)).astype(bf16)
                    far = dot(zf[:slices, :], stack(sd, st)).astype(bf16)
                    for e in range(encodings):
                        at = ((half * group + k) * encodings + e) * slices
                        for j, x in enumerate((close[:slices], close[slices:], far)):
                            product[at : at + slices, j * LANE : (j + 1) * LANE] = x[:, e * LANE : (e + 1) * LANE]
            q = dot(product[...], wi[...])
            sums = [[0.0, 0.0, 0.0] for _ in range(encodings)]
            for half, coil_ref in ((0, own_ref), (1, other_ref)):
                for k in range(group):
                    ca, cb, dr, di = coil_lanes(coil_ref, 0, k)
                    for e in range(encodings):
                        at = ((half * group + k) * encodings + e) * slices
                        qa, qb, qd, qt = (q[at : at + slices, j * LANE : (j + 1) * LANE] for j in range(4))
                        sums[e][0] += ca * qa + cb * qb
                        sums[e][1] += ca * qb - cb * qa
                        sums[e][2] += dr * qd - di * qt
            for e in range(encodings):
                for j in range(3):
                    at = e * WIDE + j * LANE
                    out_ref[:, at : at + LANE] += sums[e][j]

        one_step()

    arrays = [spectrum, own, other, column_inv, depth_fwd, depth_inv]
    coil_spec = pl.BlockSpec((1,) + own.shape[1:], lambda g: (g, 0, 0))
    spectrum_spec = pl.BlockSpec((2 * group, slices, wide), lambda g: (g, 0, 0))
    out = pltpu.HBM((slices, width), f32)
    return call(
        kernel,
        2 * 10**9,
        grid=(steps,),
        in_specs=[spectrum_spec, coil_spec, coil_spec, *(whole(a) for a in arrays[3:])],
        out_specs=whole(out),
        out_shape=out,
        scratch_shapes=[pltpu.VMEM((2 * group * encodings * slices, WIDE), bf16)],
    )(distant(spectrum), *arrays[1:])


def finish(norms_one, norms_two, data, sampling, slab_one, rows, last, readout):
    encodings, nrows, slices, lines = data.shape[1:]

    def kernel(norm_one, norm_two, data_ref, mask_ref, slab, keep, one, two, last_ref, out, image):
        lo = lax.axis_index("lo")
        alphas = step_length(norm_one), step_length(norm_two)
        for j, rows_ref in enumerate((keep, one, two)):
            r = jnp.where(lax.rem(lo, 2) == 0, j, nrows - 1 - j)
            for e in range(encodings):
                weight = mask_ref[e].astype(f32)
                real, imag = (-(data_ref[c, e, r].astype(f32) * weight) for c in range(2))
                a, b, d = (
                    alphas[0] * rows_ref[slices + 16 :, (2 * k + e) * LANE : (2 * k + e + 1) * LANE].astype(f32)
                    + alphas[1] * rows_ref[:slices, (2 * k + e) * LANE : (2 * k + e + 1) * LANE].astype(f32)
                    for k in range(3)
                )
                out[0, e, r, :, :LANE] = real[:, :LANE] - a
                out[1, e, r, :, :LANE] = imag[:, :LANE] - b
                out[0, e, r, :, LANE:] = real[:, LANE:] - d[:, :HALF]
                out[1, e, r, :, LANE:] = imag[:, LANE:] - swapped(d)[:, :HALF]
        for j in range(readout):
            x = lax.bitwise_xor(lo, j)
            for e in range(encodings):
                for k in range(3):
                    at = e * WIDE + k * LANE
                    if j < 3:
                        step = (keep, one, two)[j][slices : slices + 16, at : at + LANE]
                    else:
                        step = last_ref[:, at : at + LANE]
                    value = -alphas[0] * slab[x, :, at : at + LANE] - alphas[1] * step.astype(f32)[:8]
                    if k < 2:
                        image[k, e, x, :, :LANE] = value[:2]
                    else:
                        image[0, e, x, :, LANE:] = value[:2, :HALF]
                        image[1, e, x, :, LANE:] = swapped(value)[:2, :HALF]

    return call(
        kernel,
        10**7,
        in_specs=[VMEM] * 9,
        out_specs=[VMEM, VMEM],
        out_shape=[
            jax.ShapeDtypeStruct(data.shape, f32),
            jax.ShapeDtypeStruct((2, encodings, readout, 2, lines), f32),
        ],
    )(norms_one, norms_two, data, sampling, slab_one, *rows, last)


def reconstruct(kspace_data, coil_maps, sampling):
    encodings = kspace_data.shape[2]
    rows = kspace_data.shape[3]
    slices = kspace_data.shape[4]
    coils, readout, zdepth, lines = coil_maps.shape[1:]
    nhi, nlo = lax.axis_size("hi"), lax.axis_size("lo")
    nphase, ncore = lax.axis_size("phase"), lax.axis_size("enc")
    slabs = nhi * nlo
    group = coils // (nphase * ncore)
    assert (nlo, readout, rows, zdepth, lines, slices) == (4, 4, 3, 2, LANE + HALF, 2 * slabs)
    assert group == rows and group * nhi == coils and nphase * ncore == nhi and ncore == 2
    column_fwd, column_inv = column_table(lines, -1.0), column_table(lines, 1.0)
    depth_fwd, depth_inv = depth_table(slices, -1.0), depth_table(slices, 1.0)
    tables = (column_fwd, column_inv, depth_fwd, depth_inv)
    sampling = sampling[0]
    data = kspace_data[:, 0]

    def round_ring(value):
        value = value.reshape(slabs, zdepth, -1)
        return lax.all_to_all(value, ("hi", "lo"), 0, 0, tiled=True).reshape(slices, -1)

    packed = depart(data, sampling, coil_maps, depth_inv, nhi, group)
    packed = round_ring(packed)
    coil_rows = coil_maps.reshape(2, slabs, rows, zdepth, lines).transpose(2, 0, 1, 3, 4)
    coil_rows = coil_rows.reshape(rows, 2, slices, lines)
    slab_one, spread = slab_gradient(packed, coil_rows, column_inv, encodings, nhi)
    one = round_ring(spread)
    own = lax.all_gather(packed[:, encodings * rows * WIDE :], "phase")
    other = lax.ppermute(own, "enc", [(i, (i + 1) % ncore) for i in range(ncore)])

    up = [(i, (i + 1) % nphase) for i in range(nphase)]
    before = lax.ppermute(one, "phase", up)
    after = lax.ppermute(one, "phase", [(j, i) for i, j in up])

    def total(norms):
        return lax.all_to_all(norms, ("lo", "phase", "enc"), 0, 0, tiled=True)

    members = nlo * nphase * ncore

    def swap(value, j):
        return lax.ppermute(value, "lo", [(i, i ^ j) for i in range(nlo)])

    *rows_one, norms, spectrum = forward_step(one, (), sampling, own, other, tables, members, False)
    norms_one = total(norms)
    normal = adjoint_step(spectrum, own, other, tables, one.shape[1])
    extra = (norms_one, before, after, normal, *rows_one)
    *rows_two, norms, last = forward_step(one, extra, sampling, own, other, tables, members, True)
    near = swap(rows_two[1], 1)
    far = swap(rows_two[2], 2)
    norms_two = total(norms)
    last = swap(last, 3)
    got = [rows_two[0], near, far]
    residual, image = finish(norms_one, norms_two, data, sampling, slab_one, got, last, readout)
    return (image[:, None], residual[:, None])


def solution(mesh):
    names = dict(mesh.shape)
    nlo = 4
    grid = Mesh(
        mesh.devices.reshape(names["pat"], names["slab"] // nlo, nlo, names["phase"], names["enc"]),
        ("pat", "hi", "lo", "phase", "enc"),
    )
    slab = ("hi", "lo")
    in_specs = (
        P("pat", "phase", "enc", slab, None, None),
        P("pat", None, None, slab, None),
        P("phase", "enc", "pat", None),
    )
    out_specs = (
        P("pat", "phase", "enc", None, slab, None),
        P("pat", "phase", "enc", slab, None, None),
    )
    return jax.shard_map(reconstruct, mesh=grid, in_specs=in_specs, out_specs=out_specs, check_vma=False)
```
